8 devices in a mesh: dp: 1 (over z), tp: 2 (over y), sp: 4 (over x, core).
Axes of the slice: x: 2, y: 2, z: 1, core: 2. Of those that a mesh axis runs over, the one named last changes fastest.
Arguments:
- hidden: bfloat16 [512, 4096], P('dp')
- ln_gain: bfloat16 [4096], replicated
- ln_bias: bfloat16 [4096], replicated
- w_q: bfloat16 [4096, 6144], P(None, 'tp')
- w_k: bfloat16 [4096, 1024], P(None, 'tp')
- w_v: bfloat16 [4096, 1024], P(None, 'tp')
- w_o: bfloat16 [6144, 4096], P('tp')
- k_cache: bfloat16 [512, 512, 8, 128], P('dp', 'sp', 'tp')
- v_cache: bfloat16 [512, 512, 8, 128], P('dp', 'sp', 'tp')
- lengths: int32 [512], P('dp')
Outputs:
- output 1: bfloat16 [512, 4096], P('dp')
- output 2: bfloat16 [512, 8, 128], P('dp', 'tp')
- output 3: bfloat16 [512, 8, 128], P('dp', 'tp')
All inputs are finite; a program needn't handle non-finite values.
Results may differ from the reference program's by a relative error of at most 0.00412719.
Values sent between devices are 32-bit elements.
A program may use at most 1 GiB of HBM per device.

```python
import jax
import jax.numpy as jnp
from jax import lax

D_MODEL = 4096
Q_HEADS = 48
KV_HEADS = 8
HEAD_DIM = 128
BATCH_ROWS = 512
SEQ_LEN = 512
GROUP_SIZE = Q_HEADS // KV_HEADS
ROT_DIM = HEAD_DIM // 2


def norm_one_plus(hidden, ln_gain, ln_bias):
    wide = hidden.astype(jnp.float32)
    row_mean = jnp.mean(wide, axis=-1, keepdims=True)
    centred = wide - row_mean
    row_var = jnp.mean(centred * centred, axis=-1, keepdims=True)
    scaled = centred * lax.rsqrt(row_var + 1e-5)
    return (scaled * (1.0 + ln_gain.astype(jnp.float32)) + ln_bias.astype(jnp.float32)).astype(jnp.bfloat16)


def rotate_first(head_vecs, rot_pos):
    half_rot = ROT_DIM // 2
    inv_freq = 10000.0 ** (-2.0 * jnp.arange(half_rot, dtype=jnp.float32) / ROT_DIM)
    rot_angle = rot_pos.astype(jnp.float32)[..., None] * inv_freq
    cos_part = jnp.cos(rot_angle)
    sin_part = jnp.sin(rot_angle)
    lead_part = head_vecs[..., :half_rot]
    tail_part = head_vecs[..., half_rot:ROT_DIM]
    return jnp.concatenate([lead_part * cos_part - tail_part * sin_part, tail_part * cos_part + lead_part * sin_part, head_vecs[..., ROT_DIM:]], axis=-1)


def setup_inputs(seed: int = 0, part: int = 0) -> dict:
    shared_keys = jax.random.split(jax.random.key(seed), 6)
    part_keys = jax.random.split(jax.random.fold_in(jax.random.key(seed), part), 6)
    q_width = Q_HEADS * HEAD_DIM
    kv_width = KV_HEADS * HEAD_DIM
    seg_count = 16
    seg_len = SEQ_LEN // seg_count
    hidden = jax.random.normal(part_keys[0], (BATCH_ROWS, D_MODEL), jnp.float32)
    ln_gain = 0.5 * jax.random.normal(shared_keys[0], (D_MODEL,), jnp.float32)
    ln_bias = 0.5 * jax.random.normal(shared_keys[1], (D_MODEL,), jnp.float32)
    w_q = jax.random.normal(shared_keys[2], (D_MODEL, q_width), jnp.float32) * D_MODEL ** -0.5
    w_k = jax.random.normal(shared_keys[3], (D_MODEL, kv_width), jnp.float32) * D_MODEL ** -0.5
    w_v = jax.random.normal(shared_keys[4], (D_MODEL, kv_width), jnp.float32) * D_MODEL ** -0.5
    w_o = jax.random.normal(shared_keys[5], (q_width, D_MODEL), jnp.float32) * q_width ** -0.5
    seg_shape = (BATCH_ROWS, seg_count, 1, KV_HEADS, HEAD_DIM)
    full_shape = (BATCH_ROWS, seg_count, seg_len, KV_HEADS, HEAD_DIM)
    cache_shape = (BATCH_ROWS, SEQ_LEN, KV_HEADS, HEAD_DIM)
    k_cache = (jax.random.normal(part_keys[1], seg_shape, jnp.float32) + jax.random.normal(part_keys[2], full_shape, jnp.float32)).reshape(cache_shape)
    v_cache = (1.5 * jax.random.normal(part_keys[3], seg_shape, jnp.float32) + 0.5 * jax.random.normal(part_keys[4], full_shape, jnp.float32)).reshape(cache_shape)
    lengths = jax.random.randint(part_keys[5], (BATCH_ROWS,), SEQ_LEN // 8, SEQ_LEN, dtype=jnp.int32)
    lengths = lengths.at[0].set(SEQ_LEN - 1).at[BATCH_ROWS - 1].set(SEQ_LEN // 8)
    return {'hidden': hidden.astype(jnp.bfloat16), 'ln_gain': ln_gain.astype(jnp.bfloat16), 'ln_bias': ln_bias.astype(jnp.bfloat16), 'w_q': w_q.astype(jnp.bfloat16), 'w_k': w_k.astype(jnp.bfloat16), 'w_v': w_v.astype(jnp.bfloat16), 'w_o': w_o.astype(jnp.bfloat16), 'k_cache': k_cache.astype(jnp.bfloat16), 'v_cache': v_cache.astype(jnp.bfloat16), 'lengths': lengths}


def reference(hidden, ln_gain, ln_bias, w_q, w_k, w_v, w_o, k_cache, v_cache, lengths):
    normed = norm_one_plus(hidden, ln_gain, ln_bias)
    q_proj = jnp.dot(normed, w_q, preferred_element_type=jnp.float32).reshape(BATCH_ROWS, KV_HEADS, GROUP_SIZE, HEAD_DIM)
    queries = rotate_first(q_proj, lengths[:, None, None]).astype(jnp.bfloat16)
    k_proj = jnp.dot(normed, w_k, preferred_element_type=jnp.float32).reshape(BATCH_ROWS, KV_HEADS, HEAD_DIM)
    k_new = rotate_first(k_proj, lengths[:, None]).astype(jnp.bfloat16)
    v_new = jnp.dot(normed, w_v, preferred_element_type=jnp.float32).astype(jnp.bfloat16).reshape(BATCH_ROWS, KV_HEADS, HEAD_DIM)
    score_scale = HEAD_DIM ** -0.5
    positions = jnp.arange(SEQ_LEN)

    def one_sequence(row_args):
        q_row, k_row, v_row, k_self, v_self, length = row_args
        q_wide = q_row.astype(jnp.float32)
        scores = jnp.einsum('kgd,skd->kgs', q_wide, k_row.astype(jnp.float32)) * score_scale
        scores = jnp.where(positions < length, scores, -jnp.inf)
        self_score = jnp.einsum('kgd,kd->kg', q_wide, k_self.astype(jnp.float32)) * score_scale
        row_max = jnp.maximum(jnp.max(scores, axis=-1), self_score)
        weights = jnp.exp(scores - row_max[..., None])
        self_weight = jnp.exp(self_score - row_max)
        weight_sum = jnp.sum(weights, axis=-1) + self_weight
        narrow_w = weights.astype(jnp.bfloat16).astype(jnp.float32)
        weighted = jnp.einsum('kgs,skd->kgd', narrow_w, v_row.astype(jnp.float32))
        weighted = weighted + self_weight[..., None] * v_self.astype(jnp.float32)[:, None, :]
        return (weighted / weight_sum[..., None]).astype(jnp.bfloat16)

    context = lax.map(one_sequence, (queries, k_cache, v_cache, k_new, v_new, lengths))
    attn_out = jnp.dot(context.reshape(BATCH_ROWS, Q_HEADS * HEAD_DIM), w_o, preferred_element_type=jnp.float32)
    out = (hidden.astype(jnp.float32) + attn_out).astype(jnp.bfloat16)
    return (out, k_new, v_new)
```

```python
import functools
import jax
import jax.numpy as jnp
from jax import lax
from jax.experimental import pallas as pl
from jax.experimental.pallas import tpu as pltpu
from jax.sharding import PartitionSpec as P

MESH = pl.DeviceIdType.MESH
D = 128
G = 24
KV = 4
ROWS = 512
DM = 4096
OWN = 128
STEP = 4
NSTEP = OWN // STEP
NCH = 4
CR = OWN // NCH
SPC = NSTEP // NCH
HALF = DM // 2
NEG = -3e38
FLOOR = -1e38
SCALE2 = (128 ** -0.5) * 1.4426950408889634
F32 = jnp.float32
BF16 = jnp.bfloat16

(KD, KDS, KX, KXS, KY, KFX, KFY, KFC, KGY, KGCX, KGCY, KGCD) = range(12)


def qkv_kernel(h_ref, g_ref, b_ref, cos_ref, s1_ref, s2_ref, wq_ref, wk_ref, wv_ref,
               q_ref, k_ref, v_ref, hn, wbuf, res, kvf, sems):
    i = pl.program_id(0)
    nq = 6

    def fetch(t, slot):
        @pl.when(t < nq)
        def _():
            pltpu.make_async_copy(wq_ref.at[:, pl.ds(pl.multiple_of(t * 512, 512), 512)], wbuf.at[slot], sems.at[slot]).start()

        @pl.when(t == nq)
        def _():
            pltpu.make_async_copy(wk_ref, wbuf.at[slot], sems.at[slot]).start()

        @pl.when(t == nq + 1)
        def _():
            pltpu.make_async_copy(wv_ref, wbuf.at[slot], sems.at[slot]).start()

    @pl.when(i == 0)
    def _():
        fetch(i, 0)
        gain = 1.0 + g_ref[...].astype(F32)
        bias = b_ref[...].astype(F32)

        def norm(r, _):
            rows = pl.ds(pl.multiple_of(r * 16, 16), 16)
            wide = h_ref[rows, :].astype(F32)
            mean = jnp.mean(wide, axis=1, keepdims=True)
            cen = wide - mean
            var = jnp.mean(cen * cen, axis=1, keepdims=True)
            hn[rows, :] = ((cen * lax.rsqrt(var + 1e-5)) * gain + bias).astype(BF16)
            return 0
        lax.fori_loop(0, ROWS // 16, norm, 0)

    slot = lax.rem(i, 2)

    @pl.when(i < nq + 1)
    def _():
        fetch(i + 1, 1 - slot)
    pltpu.make_async_copy(wk_ref, wbuf.at[slot], sems.at[slot]).wait()
    res[...] = jnp.dot(hn[...], wbuf[slot], preferred_element_type=F32)

    def rope(x, rows):
        return x * cos_ref[rows, :] + pltpu.roll(x, 96, 1) * s1_ref[rows, :] + pltpu.roll(x, 32, 1) * s2_ref[rows, :]

    @pl.when(i < nq)
    def _():
        def body(r, _):
            rows = pl.ds(pl.multiple_of(r * 64, 64), 64)
            for u in range(4):
                x = rope(res[rows, u * D:(u + 1) * D], rows)
                q_ref[pl.ds(r * (64 * G) + i * 4 + u, 64, G), :] = x
            return 0
        lax.fori_loop(0, ROWS // 64, body, 0)

    @pl.when(i == nq)
    def _():
        def body(r, _):
            rows = pl.ds(pl.multiple_of(r * 64, 64), 64)
            for u in range(KV):
                kvf[pl.ds(r * (64 * KV) + u, 64, KV), :] = rope(res[rows, u * D:(u + 1) * D], rows)
            return 0
        lax.fori_loop(0, ROWS // 64, body, 0)
        k_ref[...] = kvf[...].astype(BF16)

    @pl.when(i == nq + 1)
    def _():
        def body(r, _):
            rows = pl.ds(pl.multiple_of(r * 64, 64), 64)
            for u in range(KV):
                kvf[pl.ds(r * (64 * KV) + u, 64, KV), :] = res[rows, u * D:(u + 1) * D]
            return 0
        lax.fori_loop(0, ROWS // 64, body, 0)
        v_ref[...] = kvf[...].astype(BF16)


def project(hidden, ln_gain, ln_bias, cos_t, s1_t, s2_t, w_q, w_k, w_v):
    vm = pl.BlockSpec(memory_space=pltpu.VMEM)
    hbm = pl.BlockSpec(memory_space=pl.ANY)
    return pl.pallas_call(
        qkv_kernel,
        grid=(8,),
        out_shape=(jax.ShapeDtypeStruct((ROWS * G, D), F32),
                   jax.ShapeDtypeStruct((ROWS * KV, D), BF16),
                   jax.ShapeDtypeStruct((ROWS * KV, D), BF16)),
        in_specs=[vm] * 6 + [hbm] * 3,
        out_specs=(vm, vm, vm),
        scratch_shapes=[pltpu.VMEM((ROWS, DM), BF16), pltpu.VMEM((2, DM, 512), BF16), pltpu.VMEM((ROWS, 512), F32),
                        pltpu.VMEM((ROWS * KV, D), F32), pltpu.SemaphoreType.DMA((2,))],
        compiler_params=pltpu.CompilerParams(vmem_limit_bytes=48 * 1024 * 1024, dimension_semantics=("arbitrary",)),
        cost_estimate=pl.CostEstimate(flops=2 * ROWS * DM * 4096, bytes_accessed=48 << 20, transcendentals=0),
        name="qkv",
    )(hidden, ln_gain, ln_bias, cos_t, s1_t, s2_t, w_q, w_k, w_v)


def attn_kernel(events, lens_ref, q_ref, k_ref, v_ref, qh_ref, kn_ref, vn_ref, hid_ref, wo_ref, out_ref,
                pos, acc, st, drecv, dst, cst, xrecv, xst, pout, yrecv, obuf, wo, qown, knb, vnb, knf, vnf, hid,
                ctxf, lhs, stage, lsem, osem, ssem, rsem):
    i = pl.program_id(0)
    dp = lax.axis_index("dp")
    y = lax.axis_index("tp")
    s = lax.axis_index("sp")
    x = s // 2
    c = lax.rem(s, 2)
    nx, nc, ny = 1 - x, 1 - c, 1 - y
    dev_c = (dp, y, 2 * x + nc)
    dev_x = (dp, y, 2 * nx + c)
    dev_y = (dp, ny, s)
    own = 2 * x + c
    own_x = 2 * nx + c
    base = s * 128

    def remote(kind, ch, src, dst_, dev):
        return pltpu.make_async_remote_copy(src_ref=src, dst_ref=dst_, send_sem=ssem.at[kind, ch], recv_sem=rsem.at[kind, ch],
                                            device_id=dev, device_id_type=MESH)

    locals_ = [
        (wo_ref, wo), (qh_ref.at[x, c], qown), (kn_ref.at[x, c], knb), (vn_ref.at[x, c], vnb), (hid_ref.at[x, c], hid),
    ]

    def local_copy(n):
        a, b = locals_[n]
        return pltpu.make_async_copy(a, b, lsem.at[n])

    @pl.when(i == 0)
    def _():
        sem = pltpu.get_barrier_semaphore()
        for dev in (dev_c, dev_x, dev_y):
            pl.semaphore_signal(sem, inc=1, device_id=dev, device_id_type=MESH)
        for n in range(len(locals_)):
            local_copy(n).start()
        col = lax.broadcasted_iota(jnp.int32, (48, 512), 1)
        row = lax.broadcasted_iota(jnp.int32, (48, 512), 0)
        jj = jnp.where(row >= G, row - G, row)
        head = (jj >= 6).astype(jnp.int32) + (jj >= 12).astype(jnp.int32) + (jj >= 18).astype(jnp.int32)
        pos[...] = jnp.where((col & 3) == head, col >> 2, 1 << 20)
        pl.semaphore_wait(sem, 3)

    lane = lax.broadcasted_iota(jnp.int32, (48, D), 1)
    low = lax.broadcasted_iota(jnp.int32, (48, D), 0) < G
    low1 = lax.broadcasted_iota(jnp.int32, (48, 1), 0) < G

    @pl.when(i < NSTEP)
    def _():
        ch = i // SPC
        within = lax.rem(i, SPC)
        for xo in range(2):
            for co in range(2):
                stats = jnp.where(within == 0, 0.0, st[ch, co, xo])
                for pp in range(STEP // 2):
                    q48 = q_ref[xo, co, pp * 48:(pp + 1) * 48, :]
                    qbd = jnp.concatenate([jnp.where(low, q48, 0.0), jnp.where(low, 0.0, q48)], axis=1).astype(BF16)
                    kk = jnp.concatenate([k_ref[xo, co, 2 * pp], k_ref[xo, co, 2 * pp + 1]], axis=1)
                    sc = lax.dot_general(qbd, kk, (((1,), (1,)), ((), ())), preferred_element_type=F32)
                    r0 = (2 * xo + co) * OWN + i * STEP + 2 * pp
                    lenv = jnp.where(low1, lens_ref[r0] - base, lens_ref[r0 + 1] - base)
                    sc = jnp.where(pos[...] < lenv, sc * SCALE2, NEG)
                    m = jnp.maximum(jnp.max(sc, axis=1, keepdims=True), FLOOR)
                    w = jnp.exp2(sc - m)
                    l = jnp.sum(w, axis=1, keepdims=True)
                    vv = jnp.concatenate([v_ref[xo, co, 2 * pp], v_ref[xo, co, 2 * pp + 1]], axis=1)
                    o = jnp.dot(w.astype(BF16), vv, preferred_element_type=F32)
                    at = pl.multiple_of((i * STEP + 2 * pp) * G, 2 * G)
                    acc[co, xo, pl.ds(at, G), :] = o[:G, :D]
                    acc[co, xo, pl.ds(at + G, G), :] = o[G:, D:]
                    idx = within * (STEP // 2) + pp
                    stats = jnp.where(lane == idx, m, jnp.where(lane == idx + 64, l, stats))
                st[ch, co, xo] = stats

    def pick(block, n):
        m = jnp.sum(jnp.where(lane == n, block, 0.0), axis=1, keepdims=True)
        l = jnp.sum(jnp.where(lane == n + 64, block, 0.0), axis=1, keepdims=True)
        return m, l

    def crows(ch):
        return pl.ds(ch * CR * G, CR * G)

    def c_acc(ch):
        return remote(KD, ch, acc.at[nc, :, crows(ch)], drecv.at[:, crows(ch)], dev_c)

    def c_st(ch):
        return remote(KDS, ch, st.at[ch, nc], dst.at[ch], dev_c)

    def x_acc(ch):
        return remote(KX, ch, acc.at[c, nx, crows(ch)], xrecv.at[crows(ch)], dev_x)

    def x_st(ch):
        return remote(KXS, ch, cst.at[ch, nx], xst.at[ch], dev_x)

    def y_part(ch):
        return remote(KY, ch, pout.at[ch, ny], yrecv.at[ch], dev_y)

    def piece(half, owner, ch):
        return obuf.at[half, owner, pl.ds(ch * CR, CR)]

    def gather(kind, ch, dev, half, owner):
        return remote(kind, ch, piece(half, owner, ch), piece(half, owner, ch), dev)

    own_c = 2 * x + nc
    own_xc = 2 * nx + nc

    def ev_core(ch):
        c_acc(ch).start()
        c_st(ch).start()

    def ev_x(ch):
        c_acc(ch).wait_recv()
        c_st(ch).wait_recv()

        def merge(xo, order):
            mine = st[ch, c, xo]
            theirs = dst[ch, xo]

            def body(n, out):
                rows = pl.ds(pl.multiple_of((ch * CR + 2 * n) * G, 2 * G), 2 * G)
                ma, la = pick(mine, n)
                mb, lb = pick(theirs, n)
                m = jnp.maximum(ma, mb)
                fa, fb = jnp.exp2(ma - m), jnp.exp2(mb - m)
                acc[c, xo, rows, :] = acc[c, xo, rows, :] * fa + drecv[xo, rows, :] * fb
                return jnp.where(lane == n, m, jnp.where(lane == n + 64, la * fa + lb * fb, out))
            cst[ch, xo] = lax.fori_loop(0, CR // 2, body, jnp.zeros((48, D), F32))
        merge(nx, 0)
        x_acc(ch).start()
        x_st(ch).start()
        merge(x, 1)

    def ev_proj(ch):
        if ch == 0:
            for n in range(len(locals_)):
                local_copy(n).wait()
            knf[...] = knb[...].astype(F32)
            vnf[...] = vnb[...].astype(F32)
        x_acc(ch).wait_recv()
        x_st(ch).wait_recv()
        mine = cst[ch, x]
        theirs = xst[ch]
        rr = lax.broadcasted_iota(jnp.int32, (48, 8), 0)
        cc = lax.broadcasted_iota(jnp.int32, (48, 8), 1)
        spread = ((rr >= cc * 6) & (rr < cc * 6 + 6)).astype(F32)

        def body(n, _):
            rows = pl.ds(pl.multiple_of((ch * CR + 2 * n) * G, 2 * G), 2 * G)
            krows = pl.ds(pl.multiple_of((ch * CR + 2 * n) * KV, 2 * KV), 2 * KV)
            kx = jnp.dot(spread, knf[krows, :], preferred_element_type=F32)
            vx = jnp.dot(spread, vnf[krows, :], preferred_element_type=F32)
            ms = jnp.sum(qown[rows, :].astype(BF16).astype(F32) * kx, axis=1, keepdims=True) * SCALE2
            ma, la = pick(mine, n)
            mb, lb = pick(theirs, n)
            m = jnp.maximum(jnp.maximum(ma, mb), ms)
            fa, fb, fs = jnp.exp2(ma - m), jnp.exp2(mb - m), jnp.exp2(ms - m)
            tot = la * fa + lb * fb + fs
            ctx = acc[c, x, rows, :] * fa + xrecv[rows, :] * fb + fs * vx
            ctxf[pl.ds(pl.multiple_of(n * 48, 48), 48), :] = ctx / tot
            return 0
        lax.fori_loop(0, CR // 2, body, 0)
        for j in range(G):
            lhs[:, j * D:(j + 1) * D] = ctxf[pl.ds(j, CR, G), :].astype(BF16)

        for half in range(2):
            def mm(n, _, half=half):
                cols = pl.ds(pl.multiple_of(half * HALF + n * 512, 512), 512)
                pout[ch, half, :, pl.ds(pl.multiple_of(n * 512, 512), 512)] = jnp.dot(lhs[...], wo[:, cols], preferred_element_type=F32)
                return 0
            lax.fori_loop(0, HALF // 512, mm, 0)
        y_part(ch).start()

    def ev_sum(ch):
        y_part(ch).wait_recv()
        rows = pl.ds(ch * CR, CR)

        def body(n, _):
            cols = pl.ds(pl.multiple_of(n * 512, 512), 512)
            hcols = pl.ds(pl.multiple_of(y * HALF + n * 512, 512), 512)
            obuf[y, own, rows, cols] = pout[ch, y, :, cols] + yrecv[ch, :, cols] + hid[rows, hcols].astype(F32)
            return 0
        lax.fori_loop(0, HALF // 512, body, 0)
        gather(KFX, ch, dev_x, y, own).start()
        gather(KFY, ch, dev_y, y, own).start()
        gather(KFC, ch, dev_c, y, own).start()

    def ev_fwd(ch):
        gather(KFX, ch, dev_x, y, own_x).wait_recv()
        gather(KGY, ch, dev_y, y, own_x).start()
        gather(KGCX, ch, dev_c, y, own_x).start()
        gather(KFY, ch, dev_y, ny, own).wait_recv()
        gather(KGCY, ch, dev_c, ny, own).start()

    def ev_last(ch):
        gather(KGY, ch, dev_y, ny, own_x).wait_recv()
        gather(KGCD, ch, dev_c, ny, own_x).start()

    def out_copy(ch):
        return pltpu.make_async_copy(stage.at[ch % 2], out_ref.at[:, pl.ds(ch * CR, CR)], osem.at[ch % 2])

    def ev_out(ch):
        gather(KFC, ch, dev_c, y, own_c).wait_recv()
        gather(KGCX, ch, dev_c, y, own_xc).wait_recv()
        gather(KGCY, ch, dev_c, ny, own_c).wait_recv()
        gather(KGCD, ch, dev_c, ny, own_xc).wait_recv()
        if ch >= 2:
            out_copy(ch - 2).wait()
        rows = pl.ds(ch * CR, CR)

        def body(n, _):
            for half in range(2):
                for q4 in range(4):
                    stage[ch % 2, n, :, half * HALF + q4 * 512:half * HALF + (q4 + 1) * 512] = obuf[half, n, rows, q4 * 512:(q4 + 1) * 512].astype(BF16)
            return 0
        lax.fori_loop(0, 4, body, 0)
        out_copy(ch).start()

    def ev_drain(ch):
        c_acc(ch).wait_send()
        c_st(ch).wait_send()
        x_acc(ch).wait_send()
        x_st(ch).wait_send()
        y_part(ch).wait_send()
        for kind, dev, half, owner in ((KFX, dev_x, y, own), (KFY, dev_y, y, own), (KFC, dev_c, y, own), (KGY, dev_y, y, own_x),
                                       (KGCX, dev_c, y, own_x), (KGCY, dev_c, ny, own), (KGCD, dev_c, ny, own_x)):
            gather(kind, ch, dev, half, owner).wait_send()
        if ch >= NCH - 2:
            out_copy(ch).wait()

    table = {"core": ev_core, "x": ev_x, "proj": ev_proj, "sum": ev_sum, "fwd": ev_fwd, "last": ev_last, "out": ev_out, "drain": ev_drain}
    for when, names in events:
        @pl.when(i == when)
        def _(names=names):
            for name, ch in names:
                table[name](ch)


def schedule():
    offs = (("core", 0), ("x", 2), ("proj", 10), ("sum", 16), ("fwd", 20), ("last", 23), ("out", 25))
    order = {name: n for n, (name, _) in enumerate(offs)}
    plan = {}
    for ch in range(NCH):
        first = SPC * (ch + 1) - 1
        for name, off in offs:
            plan.setdefault(min(first + off, NSTEP - 1 + 64), []).append((first + off, order[name], name, ch))
    steps = {}
    for at in sorted(plan):
        for t, o, name, ch in sorted(plan[at]):
            steps.setdefault(min(at, NSTEP), []).append((t, o, name, ch))
    out = []
    for at in sorted(steps):
        out.append((at, tuple((name, ch) for _, _, name, ch in sorted(steps[at]))))
    last = out[-1]
    out[-1] = (last[0], last[1] + tuple(("drain", ch) for ch in range(NCH)))
    return tuple(out)


def attend(lengths, q, k_cache, v_cache, kn, vn, hidden, w_o):
    hbm = pl.BlockSpec(memory_space=pl.ANY)
    hold = NSTEP - 1
    cache_spec = pl.BlockSpec((2, 2, STEP, 512, D), lambda i: (0, 0, jnp.minimum(i, hold), 0, 0))
    return pl.pallas_call(
        functools.partial(attn_kernel, schedule()),
        grid=(NSTEP + 1,),
        out_shape=jax.ShapeDtypeStruct((4, OWN, DM), BF16),
        in_specs=[pl.BlockSpec(memory_space=pltpu.SMEM),
                  pl.BlockSpec((2, 2, STEP * G, D), lambda i: (0, 0, jnp.minimum(i, hold), 0)),
                  cache_spec, cache_spec, hbm, hbm, hbm, hbm, hbm],
        out_specs=hbm,
        scratch_shapes=[
            pltpu.VMEM((48, 512), jnp.int32),
            pltpu.VMEM((2, 2, OWN * G, D), F32),
            pltpu.VMEM((NCH, 2, 2, 48, D), F32),
            pltpu.VMEM((2, OWN * G, D), F32),
            pltpu.VMEM((NCH, 2, 48, D), F32),
            pltpu.VMEM((NCH, 2, 48, D), F32),
            pltpu.VMEM((OWN * G, D), F32),
            pltpu.VMEM((NCH, 48, D), F32),
            pltpu.VMEM((NCH, 2, CR, HALF), F32),
            pltpu.VMEM((NCH, CR, HALF), F32),
            pltpu.VMEM((2, 4, OWN, HALF), F32),
            pltpu.VMEM((G * D, DM), BF16),
            pltpu.VMEM((OWN * G, D), F32),
            pltpu.VMEM((OWN * KV, D), BF16),
            pltpu.VMEM((OWN * KV, D), BF16),
            pltpu.VMEM((OWN * KV, D), F32),
            pltpu.VMEM((OWN * KV, D), F32),
            pltpu.VMEM((OWN, DM), BF16),
            pltpu.VMEM((CR * G, D), F32),
            pltpu.VMEM((CR, G * D), BF16),
            pltpu.VMEM((2, 4, CR, DM), BF16),
            pltpu.SemaphoreType.DMA((5,)),
            pltpu.SemaphoreType.DMA((2,)),
            pltpu.SemaphoreType.DMA((12, NCH)),
            pltpu.SemaphoreType.DMA((12, NCH)),
        ],
        compiler_params=pltpu.CompilerParams(vmem_limit_bytes=67043328, collective_id=0, has_side_effects=True,
                                             dimension_semantics=("arbitrary",)),
        cost_estimate=pl.CostEstimate(flops=10 ** 10, bytes_accessed=170 << 20, transcendentals=0),
        name="attend",
    )(lengths, q, k_cache, v_cache, q, kn, vn, hidden, w_o)


def solution(mesh):
    def local_step(hidden, ln_gain, ln_bias, w_q, w_k, w_v, w_o, k_cache, v_cache, lengths):
        half = D // 4
        inv = 10000.0 ** (-2.0 * jnp.arange(half, dtype=F32) / (D // 2))
        ang = lengths.astype(F32)[:, None] * inv
        cos, sin = jnp.cos(ang), jnp.sin(ang)
        zero = jnp.zeros_like(sin)
        cos_t = jnp.concatenate([cos, cos, jnp.ones((ROWS, 2 * half), F32)], axis=1)
        s1_t = jnp.concatenate([-sin, zero, zero, zero], axis=1)
        s2_t = jnp.concatenate([zero, sin, zero, zero], axis=1)
        q, kn, vn = project(hidden, ln_gain.reshape(1, DM), ln_bias.reshape(1, DM), cos_t, s1_t, s2_t, w_q, w_k, w_v)
        out = attend(lengths, q.reshape(2, 2, OWN * G, D),
                     k_cache.reshape(2, 2, OWN, 512, D), v_cache.reshape(2, 2, OWN, 512, D),
                     kn.reshape(2, 2, OWN * KV, D), vn.reshape(2, 2, OWN * KV, D),
                     hidden.reshape(2, 2, OWN, DM), w_o)
        return out.reshape(ROWS, DM), kn.reshape(ROWS, KV, D), vn.reshape(ROWS, KV, D)

    row_spec = P('dp', None)
    cache_spec = P('dp', 'sp', 'tp', None)
    head_spec = P('dp', 'tp', None)
    return jax.shard_map(local_step, mesh=mesh, in_specs=(row_spec, P(None), P(None), P(None, 'tp'), P(None, 'tp'), P(None, 'tp'), P('tp', None), cache_spec, cache_spec, P('dp')), out_specs=(row_spec, head_spec, head_spec), check_vma=False)
```

```python
import functools
import jax
import jax.numpy as jnp
from jax import lax
from jax.experimental import pallas as pl
from jax.experimental.pallas import tpu as pltpu
from jax.sharding import PartitionSpec as P

MESH = pl.DeviceIdType.MESH
D = 128
G = 24
KV = 4
ROWS = 512
DM = 4096
OWN = 128
STEP = 4
NSTEP = OWN // STEP
NCH = 8
CR = OWN // NCH
SPC = NSTEP // NCH
HALF = DM // 2
NEG = -3e38
FLOOR = -1e38
SCALE2 = (128 ** -0.5) * 1.4426950408889634
F32 = jnp.float32
BF16 = jnp.bfloat16

(KD, KDS, KX, KXS, KC, KY, KFX, KFY, KFC, KGY, KGCX, KGCY, KGCD) = range(13)
NKIND = 13
NP = CR // 2


def qkv_kernel(h_ref, g_ref, b_ref, cos_ref, s1_ref, s2_ref, wq_ref, wk_ref, wv_ref,
               q_ref, k_ref, v_ref, hn, wbuf, res, kvf, sems):
    i = pl.program_id(0)
    nq = 6

    def fetch(t, slot):
        @pl.when(t < nq)
        def _():
            pltpu.make_async_copy(wq_ref.at[:, pl.ds(pl.multiple_of(t * 512, 512), 512)], wbuf.at[slot], sems.at[slot]).start()

        @pl.when(t == nq)
        def _():
            pltpu.make_async_copy(wk_ref, wbuf.at[slot], sems.at[slot]).start()

        @pl.when(t == nq + 1)
        def _():
            pltpu.make_async_copy(wv_ref, wbuf.at[slot], sems.at[slot]).start()

    @pl.when(i == 0)
    def _():
        fetch(i, 0)
        gain = 1.0 + g_ref[...].astype(F32)
        bias = b_ref[...].astype(F32)

        def norm(r, _):
            rows = pl.ds(pl.multiple_of(r * 16, 16), 16)
            wide = h_ref[rows, :].astype(F32)
            mean = jnp.mean(wide, axis=1, keepdims=True)
            cen = wide - mean
            var = jnp.mean(cen * cen, axis=1, keepdims=True)
            hn[rows, :] = ((cen * lax.rsqrt(var + 1e-5)) * gain + bias).astype(BF16)
            return 0
        lax.fori_loop(0, ROWS // 16, norm, 0)

    slot = lax.rem(i, 2)

    @pl.when(i < nq + 1)
    def _():
        fetch(i + 1, 1 - slot)
    pltpu.make_async_copy(wk_ref, wbuf.at[slot], sems.at[slot]).wait()
    res[...] = jnp.dot(hn[...], wbuf[slot], preferred_element_type=F32)

    def rope(x, rows):
        return x * cos_ref[rows, :] + pltpu.roll(x, 96, 1) * s1_ref[rows, :] + pltpu.roll(x, 32, 1) * s2_ref[rows, :]

    @pl.when(i < nq)
    def _():
        def body(r, _):
            rows = pl.ds(pl.multiple_of(r * 64, 64), 64)
            for u in range(4):
                x = rope(res[rows, u * D:(u + 1) * D], rows)
                q_ref[pl.ds(r * (64 * G) + i * 4 + u, 64, G), :] = x
            return 0
        lax.fori_loop(0, ROWS // 64, body, 0)

    @pl.when(i == nq)
    def _():
        def body(r, _):
            rows = pl.ds(pl.multiple_of(r * 64, 64), 64)
            for u in range(KV):
                kvf[pl.ds(r * (64 * KV) + u, 64, KV), :] = rope(res[rows, u * D:(u + 1) * D], rows)
            return 0
        lax.fori_loop(0, ROWS // 64, body, 0)
        k_ref[...] = kvf[...].astype(BF16)

    @pl.when(i == nq + 1)
    def _():
        def body(r, _):
            rows = pl.ds(pl.multiple_of(r * 64, 64), 64)
            for u in range(KV):
                kvf[pl.ds(r * (64 * KV) + u, 64, KV), :] = res[rows, u * D:(u + 1) * D]
            return 0
        lax.fori_loop(0, ROWS // 64, body, 0)
        v_ref[...] = kvf[...].astype(BF16)


def project(hidden, ln_gain, ln_bias, cos_t, s1_t, s2_t, w_q, w_k, w_v):
    vm = pl.BlockSpec(memory_space=pltpu.VMEM)
    hbm = pl.BlockSpec(memory_space=pl.ANY)
    return pl.pallas_call(
        qkv_kernel,
        grid=(8,),
        out_shape=(jax.ShapeDtypeStruct((ROWS * G, D), F32),
                   jax.ShapeDtypeStruct((ROWS * KV, D), BF16),
                   jax.ShapeDtypeStruct((ROWS * KV, D), BF16)),
        in_specs=[vm] * 6 + [hbm] * 3,
        out_specs=(vm, vm, vm),
        scratch_shapes=[pltpu.VMEM((ROWS, DM), BF16), pltpu.VMEM((2, DM, 512), BF16), pltpu.VMEM((ROWS, 512), F32),
                        pltpu.VMEM((ROWS * KV, D), F32), pltpu.SemaphoreType.DMA((2,))],
        compiler_params=pltpu.CompilerParams(vmem_limit_bytes=48 * 1024 * 1024, dimension_semantics=("arbitrary",)),
        cost_estimate=pl.CostEstimate(flops=2 * ROWS * DM * 4096, bytes_accessed=48 << 20, transcendentals=0),
        name="qkv",
    )(hidden, ln_gain, ln_bias, cos_t, s1_t, s2_t, w_q, w_k, w_v)


def attn_kernel(events, lens_ref, q_ref, k_ref, v_ref, qh_ref, kn_ref, vn_ref, hid_ref, wo_ref, out_ref,
                pos, acc, st, drecv, dst, cst, sst, xrecv, xst, pout, yrecv, obuf, wo, qown, knb, vnb, knf, vnf, hid,
                ctxf, lhs, stage, scr, sms, lsem, osem, ssem, rsem):
    i = pl.program_id(0)
    dp = lax.axis_index("dp")
    y = lax.axis_index("tp")
    s = lax.axis_index("sp")
    x = s // 2
    c = lax.rem(s, 2)
    nx, nc, ny = 1 - x, 1 - c, 1 - y
    dev_c = (dp, y, 2 * x + nc)
    dev_x = (dp, y, 2 * nx + c)
    dev_y = (dp, ny, s)
    own, own_x, own_y, own_xy = 2 * x + y, 2 * nx + y, 2 * x + ny, 2 * nx + ny
    base = s * 128

    def remote(kind, ch, src, dst_, dev):
        return pltpu.make_async_remote_copy(src_ref=src, dst_ref=dst_, send_sem=ssem.at[kind, ch], recv_sem=rsem.at[kind, ch],
                                            device_id=dev, device_id_type=MESH)

    locals_ = [
        (wo_ref.at[:, pl.ds(pl.multiple_of(c * HALF, HALF), HALF)], wo), (qh_ref.at[x, c], qown), (kn_ref.at[x, c], knb), (vn_ref.at[x, c], vnb), (hid_ref.at[x, y, :, pl.ds(pl.multiple_of(c * HALF, HALF), HALF)], hid),
    ]

    def local_copy(n):
        a, b = locals_[n]
        return pltpu.make_async_copy(a, b, lsem.at[n])

    @pl.when(i == 0)
    def _():
        sem = pltpu.get_barrier_semaphore()
        for dev in (dev_c, dev_x, dev_y):
            pl.semaphore_signal(sem, inc=1, device_id=dev, device_id_type=MESH)
        col = lax.broadcasted_iota(jnp.int32, (48, 512), 1)
        row = lax.broadcasted_iota(jnp.int32, (48, 512), 0)
        jj = jnp.where(row >= G, row - G, row)
        head = (jj >= 6).astype(jnp.int32) + (jj >= 12).astype(jnp.int32) + (jj >= 18).astype(jnp.int32)
        pos[...] = jnp.where((col & 3) == head, col >> 2, 1 << 20)
        pl.semaphore_wait(sem, 3)

    @pl.when(i == 1)
    def _():
        for n in range(len(locals_)):
            local_copy(n).start()

    lane = lax.broadcasted_iota(jnp.int32, (48, D), 1)
    low = lax.broadcasted_iota(jnp.int32, (48, D), 0) < G
    low1 = lax.broadcasted_iota(jnp.int32, (48, 1), 0) < G

    @pl.when(i < NSTEP)
    def _():
        for xo in range(2):
            for co in range(2):
                for pp in range(STEP // 2):
                    q48 = q_ref[xo, co, pp * 48:(pp + 1) * 48, :]
                    qbd = jnp.concatenate([jnp.where(low, q48, 0.0), jnp.where(low, 0.0, q48)], axis=1).astype(BF16)
                    kk = jnp.concatenate([k_ref[xo, co, 2 * pp], k_ref[xo, co, 2 * pp + 1]], axis=1)
                    sc = lax.dot_general(qbd, kk, (((1,), (1,)), ((), ())), preferred_element_type=F32)
                    r0 = (2 * xo + co) * OWN + i * STEP + 2 * pp
                    lenv = jnp.where(low1, lens_ref[r0] - base, lens_ref[r0 + 1] - base)
                    scr[(xo * 2 + co) * (STEP // 2) + pp] = jnp.where(pos[...] < lenv, sc * SCALE2, NEG)

    @pl.when(i < NSTEP)
    def _():
        ch = i // SPC
        within = lax.rem(i, SPC)
        for xo in range(2):
            for co in range(2):
                stats = jnp.where(within == 0, 0.0, st[ch, co, xo])
                for pp in range(STEP // 2):
                    sc = scr[(xo * 2 + co) * (STEP // 2) + pp]
                    m = jnp.maximum(jnp.max(sc, axis=1, keepdims=True), FLOOR)
                    w = jnp.exp2(sc - m)
                    l = jnp.sum(w, axis=1, keepdims=True)
                    vv = jnp.concatenate([v_ref[xo, co, 2 * pp], v_ref[xo, co, 2 * pp + 1]], axis=1)
                    o = jnp.dot(w.astype(BF16), vv, preferred_element_type=F32)
                    at = pl.multiple_of((i * STEP + 2 * pp) * G, 2 * G)
                    acc[co, xo, pl.ds(at, G), :] = o[:G, :D]
                    acc[co, xo, pl.ds(at + G, G), :] = o[G:, D:]
                    idx = within * (STEP // 2) + pp
                    stats = jnp.where(lane == idx, m, jnp.where(lane == idx + NP, l, stats))
                st[ch, co, xo] = stats

    def pick(block, n):
        return jnp.sum(jnp.where(lane == n, block, 0.0), axis=1, keepdims=True)

    def sums(block):
        return pltpu.roll(block, D - NP, 1)

    def crows(ch):
        return pl.ds(ch * CR * G, CR * G)

    def c_acc(ch):
        return remote(KD, ch, acc.at[nc, :, crows(ch)], drecv.at[:, crows(ch)], dev_c)

    def c_st(ch):
        return remote(KDS, ch, st.at[ch, nc], dst.at[ch], dev_c)

    def x_acc(ch):
        return remote(KX, ch, acc.at[c, nx, crows(ch)], xrecv.at[crows(ch)], dev_x)

    def x_st(ch):
        return remote(KXS, ch, sst.at[ch], xst.at[ch], dev_x)

    def y_part(ch):
        return remote(KY, ch, pout.at[ch % 4, ny], yrecv.at[ch], dev_y)

    def ctx_copy(ch):
        return remote(KC, ch, ctxf.at[ch, c], ctxf.at[ch, c], dev_c)

    def ctx_in(ch):
        return remote(KC, ch, ctxf.at[ch, nc], ctxf.at[ch, nc], dev_c)

    def piece(half, owner, ch):
        return obuf.at[half, owner, pl.ds(ch * CR, CR)]

    def gather(kind, ch, dev, half, owner):
        return remote(kind, ch, piece(half, owner, ch), piece(half, owner, ch), dev)

    def ev_core(ch):
        c_acc(ch).start()
        c_st(ch).start()

    def pairs(ch, body, init):
        def four(t, carry):
            for u in range(4):
                n = t * 4 + u
                rows = pl.ds(pl.multiple_of((ch * CR + 2 * n) * G, 2 * G), 2 * G)
                carry = body(n, rows, carry)
            return carry
        return lax.fori_loop(0, CR // 8, four, init)

    def spread(ref, ch, n):
        krows = pl.ds(pl.multiple_of((ch * CR + 2 * n) * KV, 2 * KV), 2 * KV)
        rr = lax.broadcasted_iota(jnp.int32, (48, 8), 0)
        cc = lax.broadcasted_iota(jnp.int32, (48, 8), 1)
        hot = ((rr >= cc * 6) & (rr < cc * 6 + 6)).astype(F32)
        return jnp.dot(hot, ref[krows, :], preferred_element_type=F32)

    def ev_x(ch):
        c_acc(ch).wait_recv()
        c_st(ch).wait_recv()

        def merge(xo):
            a, b = st[ch, c, xo], dst[ch, xo]
            m = jnp.maximum(a, b)
            fa, fb = jnp.exp2(a - m), jnp.exp2(b - m)
            both = jnp.where(lane < NP, m, pltpu.roll(sums(a) * fa + sums(b) * fb, NP, 1))
            if xo is x:
                cst[ch] = both
            else:
                small = both[:8]
                for g in range(1, 6):
                    small = jnp.where(lane[:8] >= 16 * g, pltpu.roll(both[8 * g:8 * g + 8], 16 * g, 1), small)
                sst[ch] = small

            def body(n, rows, carry):
                acc[c, xo, rows, :] = acc[c, xo, rows, :] * pick(fa, n) + drecv[xo, rows, :] * pick(fb, n)
                return carry
            pairs(ch, body, 0)
        merge(nx)
        x_acc(ch).start()
        x_st(ch).start()
        merge(x)

    def ev_self(ch):
        if ch == 0:
            for n in range(len(locals_)):
                local_copy(n).wait()
            knf[...] = knb[...].astype(F32)
            vnf[...] = vnb[...].astype(F32)

        def body(n, rows, out):
            val = jnp.sum(qown[rows, :].astype(BF16).astype(F32) * spread(knf, ch, n), axis=1, keepdims=True)
            return jnp.where(lane == n, val, out)
        sms[ch] = pairs(ch, body, jnp.zeros((48, D), F32)) * SCALE2

    def ev_ctx(ch):
        x_acc(ch).wait_recv()
        x_st(ch).wait_recv()
        a, z, got = cst[ch], sms[ch], xst[ch]
        b = jnp.concatenate([got] + [pltpu.roll(got, D - 16 * g, 1) for g in range(1, 6)], axis=0)
        m = jnp.maximum(jnp.maximum(a, b), z)
        fa, fb, fs = jnp.exp2(a - m), jnp.exp2(b - m), jnp.exp2(z - m)
        tot = sums(a) * fa + sums(b) * fb + fs
        fa, fb, fs = fa / tot, fb / tot, fs / tot

        def body(n, rows, carry):
            ctx = acc[c, x, rows, :] * pick(fa, n) + xrecv[rows, :] * pick(fb, n) + pick(fs, n) * spread(vnf, ch, n)
            ctxf[ch, c, pl.ds(pl.multiple_of(n * 48, 48), 48), :] = ctx
            return carry
        pairs(ch, body, 0)
        ctx_copy(ch).start()

    def ev_proj(ch):
        ctx_in(ch).wait_recv()
        for j in range(G):
            for half in range(2):
                lhs[half * CR:(half + 1) * CR, j * D:(j + 1) * D] = ctxf[ch, half, pl.ds(j, CR, G), :].astype(BF16)

        def mm(n, _):
            cols = pl.ds(pl.multiple_of(n * 512, 512), 512)
            part = jnp.dot(lhs[...], wo[:, cols], preferred_element_type=F32)
            pout[ch % 4, 0, :, cols] = part[:CR]
            pout[ch % 4, 1, :, cols] = part[CR:]
            return 0
        if ch >= 4:
            y_part(ch - 4).wait_send()
        lax.fori_loop(0, HALF // 512, mm, 0)
        y_part(ch).start()

    def ev_sum(ch):
        y_part(ch).wait_recv()
        rows = pl.ds(ch * CR, CR)

        def body(n, _):
            cols = pl.ds(pl.multiple_of(n * 512, 512), 512)
            obuf[c, own, rows, cols] = pout[ch % 4, y, :, cols] + yrecv[ch, :, cols] + hid[rows, cols].astype(F32)
            return 0
        lax.fori_loop(0, HALF // 512, body, 0)
        gather(KFX, ch, dev_x, c, own).start()
        gather(KFY, ch, dev_y, c, own).start()
        gather(KFC, ch, dev_c, c, own).start()

    def ev_fwd(ch):
        gather(KFX, ch, dev_x, c, own_x).wait_recv()
        gather(KGY, ch, dev_y, c, own_x).start()
        gather(KGCX, ch, dev_c, c, own_x).start()
        gather(KFY, ch, dev_y, c, own_y).wait_recv()
        gather(KGCY, ch, dev_c, c, own_y).start()

    def ev_last(ch):
        gather(KGY, ch, dev_y, c, own_xy).wait_recv()
        gather(KGCD, ch, dev_c, c, own_xy).start()

    def out_copy(ch):
        return pltpu.make_async_copy(stage.at[ch % 2], out_ref.at[:, pl.ds(ch * CR, CR)], osem.at[ch % 2])

    def ev_out(ch):
        gather(KFC, ch, dev_c, nc, own).wait_recv()
        gather(KGCX, ch, dev_c, nc, own_x).wait_recv()
        gather(KGCY, ch, dev_c, nc, own_y).wait_recv()
        gather(KGCD, ch, dev_c, nc, own_xy).wait_recv()
        if ch >= 2:
            out_copy(ch - 2).wait()
        rows = pl.ds(ch * CR, CR)

        def body(n, _):
            for half in range(2):
                for q4 in range(4):
                    stage[ch % 2, n, :, half * HALF + q4 * 512:half * HALF + (q4 + 1) * 512] = obuf[half, n, rows, q4 * 512:(q4 + 1) * 512].astype(BF16)
            return 0
        lax.fori_loop(0, 4, body, 0)
        out_copy(ch).start()

    def ev_drain(ch):
        c_acc(ch).wait_send()
        c_st(ch).wait_send()
        x_acc(ch).wait_send()
        x_st(ch).wait_send()
        ctx_copy(ch).wait_send()
        if ch >= NCH - 4:
            y_part(ch).wait_send()
        for kind, dev, owner in ((KFX, dev_x, own), (KFY, dev_y, own), (KFC, dev_c, own), (KGY, dev_y, own_x),
                                 (KGCX, dev_c, own_x), (KGCY, dev_c, own_y), (KGCD, dev_c, own_xy)):
            gather(kind, ch, dev, c, owner).wait_send()
        if ch >= NCH - 2:
            out_copy(ch).wait()

    table = {"core": ev_core, "x": ev_x, "self": ev_self, "ctx": ev_ctx, "proj": ev_proj, "sum": ev_sum, "fwd": ev_fwd, "last": ev_last, "out": ev_out, "drain": ev_drain}
    for when, names in events:
        @pl.when(i == when)
        def _(names=names):
            for name, ch in names:
                table[name](ch)


def schedule():
    offs = (("core", 0), ("x", 1), ("self", 2), ("ctx", 6), ("proj", 7), ("sum", 10), ("fwd", 14), ("last", 17), ("out", 19))
    order = {name: n for n, (name, _) in enumerate(offs)}
    plan = {}
    for ch in range(NCH):
        first = SPC * (ch + 1) - 1
        for name, off in offs:
            plan.setdefault(min(first + off, NSTEP - 1 + 64), []).append((first + off, order[name], name, ch))
    steps = {}
    for at in sorted(plan):
        for t, o, name, ch in sorted(plan[at]):
            steps.setdefault(min(at, NSTEP), []).append((t, o, name, ch))
    out = []
    for at in sorted(steps):
        out.append((at, tuple((name, ch) for _, _, name, ch in sorted(steps[at]))))
    last = out[-1]
    out[-1] = (last[0], last[1] + tuple(("drain", ch) for ch in range(NCH)))
    return tuple(out)


def attend(lengths, q, k_cache, v_cache, kn, vn, hidden, w_o):
    hbm = pl.BlockSpec(memory_space=pl.ANY)
    hold = NSTEP - 1
    cache_spec = pl.BlockSpec((2, 2, STEP, 512, D), lambda i: (0, 0, jnp.minimum(i, hold), 0, 0))
    return pl.pallas_call(
        functools.partial(attn_kernel, schedule()),
        grid=(NSTEP + 1,),
        out_shape=jax.ShapeDtypeStruct((4, OWN, DM), BF16),
        in_specs=[pl.BlockSpec(memory_space=pltpu.SMEM),
                  pl.BlockSpec((2, 2, STEP * G, D), lambda i: (0, 0, jnp.minimum(i, hold), 0)),
                  cache_spec, cache_spec, hbm, hbm, hbm, hbm, hbm],
        out_specs=hbm,
        scratch_shapes=[
            pltpu.VMEM((48, 512), jnp.int32),
            pltpu.VMEM((2, 2, OWN * G, D), F32),
            pltpu.VMEM((NCH, 2, 2, 48, D), F32),
            pltpu.VMEM((2, OWN * G, D), F32),
            pltpu.VMEM((NCH, 2, 48, D), F32),
            pltpu.VMEM((NCH, 48, D), F32),
            pltpu.VMEM((NCH, 8, D), F32),
            pltpu.VMEM((OWN * G, D), F32),
            pltpu.VMEM((NCH, 8, D), F32),
            pltpu.VMEM((4, 2, CR, HALF), F32),
            pltpu.VMEM((NCH, CR, HALF), F32),
            pltpu.VMEM((2, 4, OWN, HALF), F32),
            pltpu.VMEM((G * D, HALF), BF16),
            pltpu.VMEM((OWN * G, D), F32),
            pltpu.VMEM((OWN * KV, D), BF16),
            pltpu.VMEM((OWN * KV, D), BF16),
            pltpu.VMEM((OWN * KV, D), F32),
            pltpu.VMEM((OWN * KV, D), F32),
            pltpu.VMEM((OWN, HALF), BF16),
            pltpu.VMEM((NCH, 2, CR * G, D), F32),
            pltpu.VMEM((2 * CR, G * D), BF16),
            pltpu.VMEM((2, 4, CR, DM), BF16),
            pltpu.VMEM((2 * STEP, 48, 512), F32),
            pltpu.VMEM((NCH, 48, D), F32),
            pltpu.SemaphoreType.DMA((5,)),
            pltpu.SemaphoreType.DMA((2,)),
            pltpu.SemaphoreType.DMA((NKIND, NCH)),
            pltpu.SemaphoreType.DMA((NKIND, NCH)),
        ],
        compiler_params=pltpu.CompilerParams(vmem_limit_bytes=67043328, collective_id=0, has_side_effects=True,
                                             dimension_semantics=("arbitrary",)),
        cost_estimate=pl.CostEstimate(flops=10 ** 10, bytes_accessed=170 << 20, transcendentals=0),
        name="attend",
    )(lengths, q, k_cache, v_cache, q, kn, vn, hidden, w_o)


def solution(mesh):
    def local_step(hidden, ln_gain, ln_bias, w_q, w_k, w_v, w_o, k_cache, v_cache, lengths):
        half = D // 4
        inv = 10000.0 ** (-2.0 * jnp.arange(half, dtype=F32) / (D // 2))
        ang = lengths.astype(F32)[:, None] * inv
        cos, sin = jnp.cos(ang), jnp.sin(ang)
        zero = jnp.zeros_like(sin)
        cos_t = jnp.concatenate([cos, cos, jnp.ones((ROWS, 2 * half), F32)], axis=1)
        s1_t = jnp.concatenate([-sin, zero, zero, zero], axis=1)
        s2_t = jnp.concatenate([zero, sin, zero, zero], axis=1)
        q, kn, vn = project(hidden, ln_gain.reshape(1, DM), ln_bias.reshape(1, DM), cos_t, s1_t, s2_t, w_q, w_k, w_v)
        out = attend(lengths, q.reshape(2, 2, OWN * G, D),
                     k_cache.reshape(2, 2, OWN, 512, D), v_cache.reshape(2, 2, OWN, 512, D),
                     kn.reshape(2, 2, OWN * KV, D), vn.reshape(2, 2, OWN * KV, D),
                     hidden.reshape(2, 2, OWN, DM), w_o)
        return out.reshape(ROWS, DM), kn.reshape(ROWS, KV, D), vn.reshape(ROWS, KV, D)

    row_spec = P('dp', None)
    cache_spec = P('dp', 'sp', 'tp', None)
    head_spec = P('dp', 'tp', None)
    return jax.shard_map(local_step, mesh=mesh, in_specs=(row_spec, P(None), P(None), P(None, 'tp'), P(None, 'tp'), P(None, 'tp'), P('tp', None), cache_spec, cache_spec, P('dp')), out_specs=(row_spec, head_spec, head_spec), check_vma=False)
```

```python
import functools
import jax
import jax.numpy as jnp
from jax import lax
from jax.experimental import pallas as pl
from jax.experimental.pallas import tpu as pltpu
from jax.sharding import PartitionSpec as P

MESH = pl.DeviceIdType.MESH
D = 128
G = 24
KV = 4
ROWS = 512
DM = 4096
OWN = 128
STEP = 4
NSTEP = OWN // STEP
NCH = 8
CR = OWN // NCH
SPC = NSTEP // NCH
NBUF = 3
XFWD = (0, 3, 6)
GROUPS = ((0, 1), (2, 3), (4, 5), (6, 7))
OFFS = {'core': 0, 'x': 1.0, 'self': 4.5, 'ctx': 5.5, 'proj': 8.0, 'sum': 14.5, 'fwd': 19.0, 'last': 28.5, 'out': 42.0}
HALF = DM // 2
NEG = -3e38
FLOOR = -1e38
SCALE2 = (128 ** -0.5) * 1.4426950408889634
F32 = jnp.float32
BF16 = jnp.bfloat16

(KD, KDS, KX, KXS, KC, KY, KFX, KFY, KFC, KGY, KGCX, KGCY, KGCD) = range(13)
NKIND = 13
NP = CR // 2


def qkv_kernel(h_ref, gb_ref, cos_ref, s1_ref, s2_ref, wq_ref, wk_ref, wv_ref,
               q_ref, k_ref, v_ref, hid, hn, wbuf, res, tb, kvr, kvf, sems, ksem, hsem, qsem, ssem, rsem):
    i = pl.program_id(0)
    rb = 128
    dp, y, s = lax.axis_index("dp"), lax.axis_index("tp"), lax.axis_index("sp")
    c = lax.rem(s, 2)
    nc = 1 - c
    peer = (dp, y, s - c + nc)

    def fetch_kv():
        cols = pl.ds(pl.multiple_of(c * 256, 256), 256)
        return (pltpu.make_async_copy(wk_ref.at[:, cols], wbuf.at[0, :, pl.ds(0, 256)], ksem.at[0]),
                pltpu.make_async_copy(wv_ref.at[:, cols], wbuf.at[0, :, pl.ds(256, 256)], ksem.at[1]))

    def fetch_q(t):
        cols = pl.ds(pl.multiple_of((3 * c + t - 1) * 512, 512), 512)
        return pltpu.make_async_copy(wq_ref.at[:, cols], wbuf.at[lax.rem(t, 2)], sems.at[lax.rem(t, 2)])

    def hcopy(r):
        rows = pl.ds(r * rb, rb)
        return pltpu.make_async_copy(h_ref.at[rows], hid.at[rows], hsem.at[r])

    def send(t):
        dst = kvr if t == 0 else q_ref.at[3 * c + t - 1]
        return pltpu.make_async_remote_copy(src_ref=tb.at[t], dst_ref=dst, send_sem=ssem.at[t], recv_sem=rsem.at[t],
                                            device_id=peer, device_id_type=MESH)

    def incoming(t):
        dst = kvr if t == 0 else q_ref.at[3 * nc + t - 1]
        return pltpu.make_async_remote_copy(src_ref=tb.at[t], dst_ref=dst, send_sem=ssem.at[t], recv_sem=rsem.at[t],
                                            device_id=peer, device_id_type=MESH)

    def keep(t):
        return pltpu.make_async_copy(tb.at[t], q_ref.at[3 * c + t - 1], qsem.at[t])

    def norm(r):
        for u in range(rb // 16):
            rows = pl.ds(r * rb + u * 16, 16)
            wide = hid[rows, :].astype(F32)
            mean = jnp.mean(wide, axis=1, keepdims=True)
            cen = wide - mean
            var = jnp.mean(cen * cen, axis=1, keepdims=True)
            hn[rows, :] = ((cen * lax.rsqrt(var + 1e-5)) * gb_ref[0:1, :] + gb_ref[1:2, :]).astype(BF16)

    def rope(x, rows):
        return x * cos_ref[rows, :] + pltpu.roll(x, 96, 1) * s1_ref[rows, :] + pltpu.roll(x, 32, 1) * s2_ref[rows, :]

    def finish(t, slot):
        for r in range(ROWS // 64):
            rows = pl.ds(r * 64, 64)
            for u in range(4):
                val = res[slot, rows, u * D:(u + 1) * D]
                tb[t, pl.ds(r * 256 + u, 64, 4), :] = val if (t == 0 and u >= 2) else rope(val, rows)

    def mul(t):
        res[t % 2] = jnp.dot(hn[...], wbuf[t % 2], preferred_element_type=F32)

    @pl.when(i == 0)
    def _():
        sem = pltpu.get_barrier_semaphore()
        pl.semaphore_signal(sem, inc=1, device_id=peer, device_id_type=MESH)
        hcopy(0).start()
        for cp in fetch_kv():
            cp.start()
        for r in range(1, 4):
            hcopy(r).start()
        fetch_q(1).start()
        hcopy(0).wait()
        norm(0)
        for cp in fetch_kv():
            cp.wait()
        for r in range(4):
            if r < 3:
                hcopy(r + 1).wait()
            res[0, r * rb:(r + 1) * rb, :] = jnp.dot(hn[r * rb:(r + 1) * rb, :], wbuf[0], preferred_element_type=F32)
            if r < 3:
                norm(r + 1)
        pl.semaphore_wait(sem, 1)

    for t in range(1, 4):
        @pl.when(i == t)
        def _(t=t):
            if t < 3:
                fetch_q(t + 1).start()
            fetch_q(t).wait()
            finish(t - 1, (t - 1) % 2)
            mul(t)
            send(t - 1).start()
            if t > 1:
                keep(t - 1).start()

    @pl.when(i == 4)
    def _():
        finish(3, 1)
        send(3).start()
        keep(3).start()
        incoming(0).wait_recv()
        for ref, off in ((k_ref, 0), (v_ref, 2)):
            for u in range(2):
                kvf[pl.ds(2 * c + u, ROWS, 4), :] = tb[0, pl.ds(off + u, ROWS, 4), :]
                kvf[pl.ds(2 * nc + u, ROWS, 4), :] = kvr[pl.ds(off + u, ROWS, 4), :]
            ref[...] = kvf[...].astype(BF16)
        for t in range(1, 4):
            keep(t).wait()
            incoming(t).wait_recv()
        for t in range(4):
            send(t).wait_send()


def project(hidden, gb, cos_t, s1_t, s2_t, w_q, w_k, w_v):
    vm = pl.BlockSpec(memory_space=pltpu.VMEM)
    hbm = pl.BlockSpec(memory_space=pl.ANY)
    return pl.pallas_call(
        qkv_kernel,
        grid=(5,),
        out_shape=(jax.ShapeDtypeStruct((6, ROWS * 4, D), F32),
                   jax.ShapeDtypeStruct((ROWS * KV, D), BF16),
                   jax.ShapeDtypeStruct((ROWS * KV, D), BF16)),
        in_specs=[hbm] + [vm] * 4 + [hbm] * 3,
        out_specs=(hbm, vm, vm),
        scratch_shapes=[pltpu.VMEM((ROWS, DM), BF16), pltpu.VMEM((ROWS, DM), BF16), pltpu.VMEM((2, DM, 512), BF16),
                        pltpu.VMEM((2, ROWS, 512), F32), pltpu.VMEM((4, ROWS * 4, D), F32), pltpu.VMEM((ROWS * 4, D), F32),
                        pltpu.VMEM((ROWS * KV, D), F32),
                        pltpu.SemaphoreType.DMA((2,)), pltpu.SemaphoreType.DMA((2,)), pltpu.SemaphoreType.DMA((4,)),
                        pltpu.SemaphoreType.DMA((4,)), pltpu.SemaphoreType.DMA((4,)), pltpu.SemaphoreType.DMA((4,))],
        compiler_params=pltpu.CompilerParams(vmem_limit_bytes=60 * 1024 * 1024, dimension_semantics=("arbitrary",),
                                             collective_id=1, has_side_effects=True),
        cost_estimate=pl.CostEstimate(flops=ROWS * DM * 4096, bytes_accessed=32 << 20, transcendentals=0),
        name="qkv",
    )(hidden, gb, cos_t, s1_t, s2_t, w_q, w_k, w_v)


def attn_kernel(events, lens_ref, q_ref, kc_ref, vc_ref, qh_ref, kn_ref, vn_ref, hid_ref, wo_ref, out_ref,
                kbuf, vbuf, pos, acc, st, drecv, dst, cst, sst, xrecv, xst, pout, yrecv, obuf, wo, qown, knb, vnb, knf, vnf, hid,
                ctxf, lhs, stage, scr, sms, csem, lsem, osem, ssem, rsem):
    i = pl.program_id(0)
    dp = lax.axis_index("dp")
    y = lax.axis_index("tp")
    s = lax.axis_index("sp")
    x = s // 2
    c = lax.rem(s, 2)
    nx, nc, ny = 1 - x, 1 - c, 1 - y
    dev_c = (dp, y, 2 * x + nc)
    dev_x = (dp, y, 2 * nx + c)
    dev_y = (dp, ny, s)
    own, own_x, own_y, own_xy = 2 * x + y, 2 * nx + y, 2 * x + ny, 2 * nx + ny
    base = s * 128

    def remote(kind, ch, src, dst_, dev):
        return pltpu.make_async_remote_copy(src_ref=src, dst_ref=dst_, send_sem=ssem.at[kind, ch], recv_sem=rsem.at[kind, ch],
                                            device_id=dev, device_id_type=MESH)

    locals_ = [
        (wo_ref.at[:, pl.ds(pl.multiple_of(c * HALF, HALF), HALF)], wo), (qh_ref.at[:, x, c], qown), (kn_ref.at[x, c], knb), (vn_ref.at[x, c], vnb), (hid_ref.at[x, y, :, pl.ds(pl.multiple_of(c * HALF, HALF), HALF)], hid),
    ]

    def local_copy(n):
        a, b = locals_[n]
        return pltpu.make_async_copy(a, b, lsem.at[n])

    def cache_copies(t):
        b = lax.rem(t, NBUF)
        blk = pl.ds(t * STEP, STEP)
        return (pltpu.make_async_copy(kc_ref.at[:, :, blk], kbuf.at[b], csem.at[0, b]),
                pltpu.make_async_copy(vc_ref.at[:, :, blk], vbuf.at[b], csem.at[1, b]))

    @pl.when(i == 0)
    def _():
        for t in range(NBUF - 1):
            for cp in cache_copies(t):
                cp.start()

    @pl.when(i < NSTEP - NBUF + 1)
    def _():
        for cp in cache_copies(i + NBUF - 1):
            cp.start()

    @pl.when(i == 0)
    def _():
        sem = pltpu.get_barrier_semaphore()
        for dev in (dev_c, dev_x, dev_y):
            pl.semaphore_signal(sem, inc=1, device_id=dev, device_id_type=MESH)
        col = lax.broadcasted_iota(jnp.int32, (48, 512), 1)
        row = lax.broadcasted_iota(jnp.int32, (48, 512), 0)
        jj = (row >> 3) * 4 + (row & 3)
        head = (jj >= 6).astype(jnp.int32) + (jj >= 12).astype(jnp.int32) + (jj >= 18).astype(jnp.int32)
        pos[...] = jnp.where((col & 3) == head, col >> 2, 1 << 20)
        pl.semaphore_wait(sem, 3)

    @pl.when(i == 1)
    def _():
        for n in range(len(locals_)):
            local_copy(n).start()

    lane = lax.broadcasted_iota(jnp.int32, (48, D), 1)
    low = (lax.broadcasted_iota(jnp.int32, (48, D), 0) & 7) < 4
    low1 = (lax.broadcasted_iota(jnp.int32, (48, 1), 0) & 7) < 4

    @pl.when(i < NSTEP)
    def _():
        for cp in cache_copies(i):
            cp.wait()
        k_ref = kbuf.at[lax.rem(i, NBUF)]
        for xo in range(2):
            for co in range(2):
                for pp in range(STEP // 2):
                    q48 = q_ref[:, xo, co, pp * 8:(pp + 1) * 8, :].reshape(48, D)
                    qbd = jnp.concatenate([jnp.where(low, q48, 0.0), jnp.where(low, 0.0, q48)], axis=1).astype(BF16)
                    kk = jnp.concatenate([k_ref[xo, co, 2 * pp], k_ref[xo, co, 2 * pp + 1]], axis=1)
                    sc = lax.dot_general(qbd, kk, (((1,), (1,)), ((), ())), preferred_element_type=F32)
                    r0 = (2 * xo + co) * OWN + i * STEP + 2 * pp
                    lenv = jnp.where(low1, lens_ref[r0] - base, lens_ref[r0 + 1] - base)
                    scr[(xo * 2 + co) * (STEP // 2) + pp] = jnp.where(pos[...] < lenv, sc * SCALE2, NEG)

    @pl.when(i < NSTEP)
    def _():
        v_ref = vbuf.at[lax.rem(i, NBUF)]
        ch = i // SPC
        within = lax.rem(i, SPC)
        for xo in range(2):
            for co in range(2):
                stats = jnp.where(within == 0, 0.0, st[ch, co, xo])
                for pp in range(STEP // 2):
                    sc = scr[(xo * 2 + co) * (STEP // 2) + pp]
                    m = jnp.maximum(jnp.max(sc, axis=1, keepdims=True), FLOOR)
                    w = jnp.exp2(sc - m)
                    l = jnp.sum(w, axis=1, keepdims=True)
                    vv = jnp.concatenate([v_ref[xo, co, 2 * pp], v_ref[xo, co, 2 * pp + 1]], axis=1)
                    o = jnp.dot(w.astype(BF16), vv, preferred_element_type=F32)
                    at = pl.multiple_of((i * STEP + 2 * pp) * G, 2 * G)
                    acc[co, xo, pl.ds(at, 2 * G), :] = jnp.where(low, o[:, :D], o[:, D:])
                    idx = within * (STEP // 2) + pp
                    stats = jnp.where(lane == idx, m, jnp.where(lane == idx + NP, l, stats))
                st[ch, co, xo] = stats

    def pick(block, n):
        return jnp.sum(jnp.where(lane == n, block, 0.0), axis=1, keepdims=True)

    def sums(block):
        return pltpu.roll(block, D - NP, 1)

    def crows(ch):
        return pl.ds(ch * CR * G, CR * G)

    def c_acc(ch):
        return remote(KD, ch, acc.at[nc, :, crows(ch)], drecv.at[:, crows(ch)], dev_c)

    def c_st(ch):
        return remote(KDS, ch, st.at[ch, nc], dst.at[ch], dev_c)

    def x_acc(ch):
        return remote(KX, ch, acc.at[c, nx, crows(ch)], xrecv.at[crows(ch)], dev_x)

    def x_st(ch):
        return remote(KXS, ch, sst.at[ch], xst.at[ch], dev_x)

    def y_part(ch):
        return remote(KY, ch, pout.at[ch % 4, ny], yrecv.at[ch], dev_y)

    def ctx_copy(ch):
        return remote(KC, ch, ctxf.at[ch, c], ctxf.at[ch, c], dev_c)

    def ctx_in(ch):
        return remote(KC, ch, ctxf.at[ch, nc], ctxf.at[ch, nc], dev_c)

    def piece(half, owner, ch):
        return obuf.at[half, owner, pl.ds(ch * CR, CR)]

    def gather(kind, ch, dev, half, owner):
        return remote(kind, ch, piece(half, owner, ch), piece(half, owner, ch), dev)

    def ev_core(ch):
        c_acc(ch).start()
        c_st(ch).start()

    def pairs(ch, body, init):
        def four(t, carry):
            for u in range(4):
                n = t * 4 + u
                rows = pl.ds(pl.multiple_of((ch * CR + 2 * n) * G, 2 * G), 2 * G)
                carry = body(n, rows, carry)
            return carry
        return lax.fori_loop(0, CR // 8, four, init)

    def spread(ref, ch, n):
        krows = pl.ds(pl.multiple_of((ch * CR + 2 * n) * KV, 2 * KV), 2 * KV)
        rr = lax.broadcasted_iota(jnp.int32, (48, 8), 0)
        cc = lax.broadcasted_iota(jnp.int32, (48, 8), 1)
        first = ((cc & 3) * 6)
        jj = (rr >> 3) * 4 + (rr & 3)
        hot = ((jj >= first) & (jj < first + 6) & (((rr >> 2) & 1) == (cc >> 2))).astype(F32)
        return jnp.dot(hot, ref[krows, :], preferred_element_type=F32)

    def ev_x(ch):
        c_acc(ch).wait_recv()
        c_st(ch).wait_recv()

        def merge(xo):
            a, b = st[ch, c, xo], dst[ch, xo]
            m = jnp.maximum(a, b)
            fa, fb = jnp.exp2(a - m), jnp.exp2(b - m)
            both = jnp.where(lane < NP, m, pltpu.roll(sums(a) * fa + sums(b) * fb, NP, 1))
            if xo is x:
                cst[ch] = both
            else:
                small = both[:8]
                for g in range(1, 6):
                    small = jnp.where(lane[:8] >= 16 * g, pltpu.roll(both[8 * g:8 * g + 8], 16 * g, 1), small)
                sst[ch] = small

            def body(n, rows, carry):
                acc[c, xo, rows, :] = acc[c, xo, rows, :] * pick(fa, n) + drecv[xo, rows, :] * pick(fb, n)
                return carry
            pairs(ch, body, 0)
        merge(nx)
        x_acc(ch).start()
        x_st(ch).start()
        merge(x)

    def ev_self(ch):
        if ch == 0:
            for n in range(len(locals_)):
                local_copy(n).wait()
            knf[...] = knb[...].astype(F32)
            vnf[...] = vnb[...].astype(F32)

        def body(n, rows, out):
            qq = qown[:, pl.ds(pl.multiple_of((ch * CR + 2 * n) * 4, 8), 8), :].reshape(48, D)
            val = jnp.sum(qq.astype(BF16).astype(F32) * spread(knf, ch, n), axis=1, keepdims=True)
            return jnp.where(lane == n, val, out)
        sms[ch] = pairs(ch, body, jnp.zeros((48, D), F32)) * SCALE2

    def ev_ctx(ch):
        x_acc(ch).wait_recv()
        x_st(ch).wait_recv()
        a, z, got = cst[ch], sms[ch], xst[ch]
        b = jnp.concatenate([got] + [pltpu.roll(got, D - 16 * g, 1) for g in range(1, 6)], axis=0)
        m = jnp.maximum(jnp.maximum(a, b), z)
        fa, fb, fs = jnp.exp2(a - m), jnp.exp2(b - m), jnp.exp2(z - m)
        tot = sums(a) * fa + sums(b) * fb + fs
        fa, fb, fs = fa / tot, fb / tot, fs / tot

        def body(n, rows, carry):
            ctx = acc[c, x, rows, :] * pick(fa, n) + xrecv[rows, :] * pick(fb, n) + pick(fs, n) * spread(vnf, ch, n)
            for k in range(3):
                lo, hi = ctx[16 * k:16 * k + 8], ctx[16 * k + 8:16 * k + 16]
                at = pl.multiple_of(n * 48 + 8 * k, 8)
                ctxf[ch, c, pl.ds(at, 8), :] = jnp.where(low[:8], lo, pltpu.roll(hi, 4, 0))
                ctxf[ch, c, pl.ds(at + G, 8), :] = jnp.where(low[:8], pltpu.roll(lo, 4, 0), hi)
            return carry
        pairs(ch, body, 0)
        ctx_copy(ch).start()

    def ev_proj(group):
        m = len(group)
        for g, ch in enumerate(group):
            ctx_in(ch).wait_recv()
            for j in range(G):
                for half in range(2):
                    lhs[pl.ds((2 * g + half) * CR, CR), j * D:(j + 1) * D] = ctxf[ch, half, pl.ds(j, CR, G), :].astype(BF16)
            if ch >= 4:
                y_part(ch - 4).wait_send()

        def mm(n, _):
            cols = pl.ds(pl.multiple_of(n * 512, 512), 512)
            part = jnp.dot(lhs[:m * 2 * CR], wo[:, cols], preferred_element_type=F32)
            for g, ch in enumerate(group):
                for half in range(2):
                    pout[ch % 4, half, :, cols] = part[(2 * g + half) * CR:(2 * g + half + 1) * CR]
            return 0
        lax.fori_loop(0, HALF // 512, mm, 0)
        for ch in group:
            y_part(ch).start()

    def ev_sum(ch):
        y_part(ch).wait_recv()
        rows = pl.ds(ch * CR, CR)

        def body(n, _):
            cols = pl.ds(pl.multiple_of(n * 512, 512), 512)
            obuf[c, own, rows, cols] = pout[ch % 4, y, :, cols] + yrecv[ch, :, cols] + hid[rows, cols].astype(F32)
            return 0
        lax.fori_loop(0, HALF // 512, body, 0)
        gather(KFX, ch, dev_x, c, own).start()
        gather(KFY, ch, dev_y, c, own).start()
        gather(KFC, ch, dev_c, c, own).start()

    def forward(ch):
        if ch in XFWD:
            return gather(KGY, ch, dev_x, c, own_y)
        return gather(KGY, ch, dev_y, c, own_x)

    def ev_fwd(ch):
        gather(KFX, ch, dev_x, c, own_x).wait_recv()
        if ch not in XFWD:
            forward(ch).start()
        gather(KGCX, ch, dev_c, c, own_x).start()
        gather(KFY, ch, dev_y, c, own_y).wait_recv()
        if ch in XFWD:
            forward(ch).start()
        gather(KGCY, ch, dev_c, c, own_y).start()

    def ev_last(ch):
        gather(KGY, ch, dev_y, c, own_xy).wait_recv()
        gather(KGCD, ch, dev_c, c, own_xy).start()

    def out_copy(ch):
        return pltpu.make_async_copy(stage.at[ch % 2], out_ref.at[:, pl.ds(ch * CR, CR)], osem.at[ch % 2])

    def ev_out(ch):
        gather(KFC, ch, dev_c, nc, own).wait_recv()
        gather(KGCX, ch, dev_c, nc, own_x).wait_recv()
        gather(KGCY, ch, dev_c, nc, own_y).wait_recv()
        gather(KGCD, ch, dev_c, nc, own_xy).wait_recv()
        if ch >= 2:
            out_copy(ch - 2).wait()
        rows = pl.ds(ch * CR, CR)

        def body(n, _):
            for half in range(2):
                for q4 in range(4):
                    stage[ch % 2, n, :, half * HALF + q4 * 512:half * HALF + (q4 + 1) * 512] = obuf[half, n, rows, q4 * 512:(q4 + 1) * 512].astype(BF16)
            return 0
        lax.fori_loop(0, 4, body, 0)
        out_copy(ch).start()

    def ev_drain(ch):
        c_acc(ch).wait_send()
        c_st(ch).wait_send()
        x_acc(ch).wait_send()
        x_st(ch).wait_send()
        ctx_copy(ch).wait_send()
        if ch >= NCH - 4:
            y_part(ch).wait_send()
        for kind, dev, owner in ((KFX, dev_x, own), (KFY, dev_y, own), (KFC, dev_c, own),
                                 (KGCX, dev_c, own_x), (KGCY, dev_c, own_y), (KGCD, dev_c, own_xy)):
            gather(kind, ch, dev, c, owner).wait_send()
        forward(ch).wait_send()
        if ch >= NCH - 2:
            out_copy(ch).wait()

    table = {"core": ev_core, "x": ev_x, "self": ev_self, "ctx": ev_ctx, "proj": ev_proj, "sum": ev_sum, "fwd": ev_fwd, "last": ev_last, "out": ev_out, "drain": ev_drain}
    for when, names in events:
        @pl.when(i == when)
        def _(names=names):
            for name, ch in names:
                table[name](ch)


def schedule():
    order = {name: n for n, name in enumerate(OFFS)}
    plan = []
    for ch in range(NCH):
        first = SPC * (ch + 1) - 1
        for name, off in OFFS.items():
            if name != "proj":
                plan.append((first + off, order[name], name, ch))
    for group in GROUPS:
        plan.append((SPC * (group[-1] + 1) - 1 + OFFS["proj"], order["proj"], "proj", group))
    plan.sort()
    steps = {}
    for at, _, name, arg in plan:
        steps.setdefault(min(int(at), NSTEP), []).append((name, arg))
    steps[NSTEP] += [("drain", ch) for ch in range(NCH)]
    return tuple((at, tuple(steps[at])) for at in sorted(steps))


def attend(lengths, q, k_cache, v_cache, kn, vn, hidden, w_o):
    hbm = pl.BlockSpec(memory_space=pl.ANY)
    hold = NSTEP - 1
    return pl.pallas_call(
        functools.partial(attn_kernel, schedule()),
        grid=(NSTEP + 1,),
        out_shape=jax.ShapeDtypeStruct((4, OWN, DM), BF16),
        in_specs=[pl.BlockSpec(memory_space=pltpu.SMEM),
                  pl.BlockSpec((6, 2, 2, STEP * 4, D), lambda i: (0, 0, 0, jnp.minimum(i, hold), 0)),
                  hbm, hbm, hbm, hbm, hbm, hbm, hbm],
        out_specs=hbm,
        scratch_shapes=[
            pltpu.VMEM((NBUF, 2, 2, STEP, 512, D), BF16),
            pltpu.VMEM((NBUF, 2, 2, STEP, 512, D), BF16),
            pltpu.VMEM((48, 512), jnp.int32),
            pltpu.VMEM((2, 2, OWN * G, D), F32),
            pltpu.VMEM((NCH, 2, 2, 48, D), F32),
            pltpu.VMEM((2, OWN * G, D), F32),
            pltpu.VMEM((NCH, 2, 48, D), F32),
            pltpu.VMEM((NCH, 48, D), F32),
            pltpu.VMEM((NCH, 8, D), F32),
            pltpu.VMEM((OWN * G, D), F32),
            pltpu.VMEM((NCH, 8, D), F32),
            pltpu.VMEM((4, 2, CR, HALF), F32),
            pltpu.VMEM((NCH, CR, HALF), F32),
            pltpu.VMEM((2, 4, OWN, HALF), F32),
            pltpu.VMEM((G * D, HALF), BF16),
            pltpu.VMEM((6, OWN * 4, D), F32),
            pltpu.VMEM((OWN * KV, D), BF16),
            pltpu.VMEM((OWN * KV, D), BF16),
            pltpu.VMEM((OWN * KV, D), F32),
            pltpu.VMEM((OWN * KV, D), F32),
            pltpu.VMEM((OWN, HALF), BF16),
            pltpu.VMEM((NCH, 2, CR * G, D), F32),
            pltpu.VMEM((4 * CR, G * D), BF16),
            pltpu.VMEM((2, 4, CR, DM), BF16),
            pltpu.VMEM((2 * STEP, 48, 512), F32),
            pltpu.VMEM((NCH, 48, D), F32),
            pltpu.SemaphoreType.DMA((2, NBUF)),
            pltpu.SemaphoreType.DMA((5,)),
            pltpu.SemaphoreType.DMA((2,)),
            pltpu.SemaphoreType.DMA((NKIND, NCH)),
            pltpu.SemaphoreType.DMA((NKIND, NCH)),
        ],
        compiler_params=pltpu.CompilerParams(vmem_limit_bytes=67043328, collective_id=0, has_side_effects=True,
                                             dimension_semantics=("arbitrary",)),
        cost_estimate=pl.CostEstimate(flops=10 ** 10, bytes_accessed=170 << 20, transcendentals=0),
        name="attend",
    )(lengths, q, k_cache, v_cache, q, kn, vn, hidden, w_o)


def solution(mesh):
    def local_step(hidden, ln_gain, ln_bias, w_q, w_k, w_v, w_o, k_cache, v_cache, lengths):
        half = D // 4
        inv = 10000.0 ** (-2.0 * jnp.arange(half, dtype=F32) / (D // 2))
        ang = lengths.astype(F32)[:, None] * inv
        cos, sin = jnp.cos(ang), jnp.sin(ang)
        zero = jnp.zeros_like(sin)
        cos_t = jnp.concatenate([cos, cos, jnp.ones((ROWS, 2 * half), F32)], axis=1)
        s1_t = jnp.concatenate([-sin, zero, zero, zero], axis=1)
        s2_t = jnp.concatenate([zero, sin, zero, zero], axis=1)
        gb = jnp.stack([1.0 + ln_gain.astype(F32), ln_bias.astype(F32)])
        q, kn, vn = project(hidden, gb, cos_t, s1_t, s2_t, w_q, w_k, w_v)
        out = attend(lengths, q.reshape(6, 2, 2, OWN * 4, D),
                     k_cache.reshape(2, 2, OWN, 512, D), v_cache.reshape(2, 2, OWN, 512, D),
                     kn.reshape(2, 2, OWN * KV, D), vn.reshape(2, 2, OWN * KV, D),
                     hidden.reshape(2, 2, OWN, DM), w_o)
        return out.reshape(ROWS, DM), kn.reshape(ROWS, KV, D), vn.reshape(ROWS, KV, D)

    row_spec = P('dp', None)
    cache_spec = P('dp', 'sp', 'tp', None)
    head_spec = P('dp', 'tp', None)
    return jax.shard_map(local_step, mesh=mesh, in_specs=(row_spec, P(None), P(None), P(None, 'tp'), P(None, 'tp'), P(None, 'tp'), P('tp', None), cache_spec, cache_spec, P('dp')), out_specs=(row_spec, head_spec, head_spec), check_vma=False)
```

```python
import functools
import jax
import jax.numpy as jnp
from jax import lax
from jax.experimental import pallas as pl
from jax.experimental.pallas import tpu as pltpu
from jax.sharding import PartitionSpec as P

MESH = pl.DeviceIdType.MESH
D = 128
G = 24
KV = 4
ROWS = 512
DM = 4096
OWN = 128
STEP = 4
NSTEP = OWN // STEP
NCH = 8
CR = OWN // NCH
SPC = NSTEP // NCH
NBUF = 3
XFWD = (0, 3, 6)
GROUPS = ((0, 1), (2, 3), (4, 5), (6, 7))
OFFS = {'core': 0, 'x': 1.0, 'self': 4.5, 'ctx': 5.5, 'proj': 8.0, 'sum': 14.5, 'fwd': 19.0, 'last': 28.5, 'out': 42.0}
HALF = DM // 2
NEG = -3e38
FLOOR = -1e38
SCALE2 = (128 ** -0.5) * 1.4426950408889634
F32 = jnp.float32
BF16 = jnp.bfloat16

(KD, KDS, KX, KXS, KC, KY, KFX, KFY, KFC, KGY, KGCX, KGCY, KGCD) = range(13)
NKIND = 13
NP = CR // 2


def qkv_kernel(h_ref, gb_ref, cos_ref, s1_ref, s2_ref, wq_ref, wk_ref, wv_ref,
               q_ref, k_ref, v_ref, hid, hn, wbuf, res, tb, kvr, kvf, sems, ksem, hsem, qsem, ssem, rsem):
    i = pl.program_id(0)
    rb = 128
    dp, y, s = lax.axis_index("dp"), lax.axis_index("tp"), lax.axis_index("sp")
    c = lax.rem(s, 2)
    nc = 1 - c
    peer = (dp, y, s - c + nc)

    def fetch_kv():
        cols = pl.ds(pl.multiple_of(c * 256, 256), 256)
        return (pltpu.make_async_copy(wk_ref.at[:, cols], wbuf.at[0, :, pl.ds(0, 256)], ksem.at[0]),
                pltpu.make_async_copy(wv_ref.at[:, cols], wbuf.at[0, :, pl.ds(256, 256)], ksem.at[1]))

    def fetch_q(t):
        cols = pl.ds(pl.multiple_of((3 * c + t - 1) * 512, 512), 512)
        return pltpu.make_async_copy(wq_ref.at[:, cols], wbuf.at[lax.rem(t, 2)], sems.at[lax.rem(t, 2)])

    def hcopy(r):
        rows = pl.ds(r * rb, rb)
        return pltpu.make_async_copy(h_ref.at[rows], hid.at[rows], hsem.at[r])

    def send(t):
        dst = kvr if t == 0 else q_ref.at[3 * c + t - 1]
        return pltpu.make_async_remote_copy(src_ref=tb.at[t], dst_ref=dst, send_sem=ssem.at[t], recv_sem=rsem.at[t],
                                            device_id=peer, device_id_type=MESH)

    def incoming(t):
        dst = kvr if t == 0 else q_ref.at[3 * nc + t - 1]
        return pltpu.make_async_remote_copy(src_ref=tb.at[t], dst_ref=dst, send_sem=ssem.at[t], recv_sem=rsem.at[t],
                                            device_id=peer, device_id_type=MESH)

    def keep(t):
        return pltpu.make_async_copy(tb.at[t], q_ref.at[3 * c + t - 1], qsem.at[t])

    def norm(r):
        for u in range(rb // 16):
            rows = pl.ds(r * rb + u * 16, 16)
            wide = hid[rows, :].astype(F32)
            mean = jnp.mean(wide, axis=1, keepdims=True)
            cen = wide - mean
            var = jnp.mean(cen * cen, axis=1, keepdims=True)
            hn[rows, :] = ((cen * lax.rsqrt(var + 1e-5)) * gb_ref[0:1, :] + gb_ref[1:2, :]).astype(BF16)

    def rope(x, rows):
        return x * cos_ref[rows, :] + pltpu.roll(x, 96, 1) * s1_ref[rows, :] + pltpu.roll(x, 32, 1) * s2_ref[rows, :]

    def finish(t, slot):
        for r in range(ROWS // 64):
            rows = pl.ds(r * 64, 64)
            for u in range(4):
                val = res[slot, rows, u * D:(u + 1) * D]
                tb[t, pl.ds(r * 256 + u, 64, 4), :] = val if (t == 0 and u >= 2) else rope(val, rows)

    def mul(t):
        res[t % 2] = jnp.dot(hn[...], wbuf[t % 2], preferred_element_type=F32)

    @pl.when(i == 0)
    def _():
        sem = pltpu.get_barrier_semaphore()
        pl.semaphore_signal(sem, inc=1, device_id=peer, device_id_type=MESH)
        hcopy(0).start()
        for cp in fetch_kv():
            cp.start()
        for r in range(1, 4):
            hcopy(r).start()
        fetch_q(1).start()
        hcopy(0).wait()
        norm(0)
        for cp in fetch_kv():
            cp.wait()
        for r in range(4):
            if r < 3:
                hcopy(r + 1).wait()
            res[0, r * rb:(r + 1) * rb, :] = jnp.dot(hn[r * rb:(r + 1) * rb, :], wbuf[0], preferred_element_type=F32)
            if r < 3:
                norm(r + 1)
        pl.semaphore_wait(sem, 1)

    for t in range(1, 4):
        @pl.when(i == t)
        def _(t=t):
            if t < 3:
                fetch_q(t + 1).start()
            fetch_q(t).wait()
            finish(t - 1, (t - 1) % 2)
            mul(t)
            send(t - 1).start()
            if t > 1:
                keep(t - 1).start()

    @pl.when(i == 4)
    def _():
        finish(3, 1)
        send(3).start()
        keep(3).start()
        incoming(0).wait_recv()
        for ref, off in ((k_ref, 0), (v_ref, 2)):
            for u in range(2):
                kvf[pl.ds(2 * c + u, ROWS, 4), :] = tb[0, pl.ds(off + u, ROWS, 4), :]
                kvf[pl.ds(2 * nc + u, ROWS, 4), :] = kvr[pl.ds(off + u, ROWS, 4), :]
            ref[...] = kvf[...].astype(BF16)
        for t in range(1, 4):
            keep(t).wait()
            incoming(t).wait_recv()
        for t in range(4):
            send(t).wait_send()


def project(hidden, gb, cos_t, s1_t, s2_t, w_q, w_k, w_v):
    vm = pl.BlockSpec(memory_space=pltpu.VMEM)
    hbm = pl.BlockSpec(memory_space=pl.ANY)
    return pl.pallas_call(
        qkv_kernel,
        grid=(5,),
        out_shape=(jax.ShapeDtypeStruct((6, ROWS * 4, D), F32),
                   jax.ShapeDtypeStruct((ROWS * KV, D), BF16),
                   jax.ShapeDtypeStruct((ROWS * KV, D), BF16)),
        in_specs=[hbm] + [vm] * 4 + [hbm] * 3,
        out_specs=(hbm, vm, vm),
        scratch_shapes=[pltpu.VMEM((ROWS, DM), BF16), pltpu.VMEM((ROWS, DM), BF16), pltpu.VMEM((2, DM, 512), BF16),
                        pltpu.VMEM((2, ROWS, 512), F32), pltpu.VMEM((4, ROWS * 4, D), F32), pltpu.VMEM((ROWS * 4, D), F32),
                        pltpu.VMEM((ROWS * KV, D), F32),
                        pltpu.SemaphoreType.DMA((2,)), pltpu.SemaphoreType.DMA((2,)), pltpu.SemaphoreType.DMA((4,)),
                        pltpu.SemaphoreType.DMA((4,)), pltpu.SemaphoreType.DMA((4,)), pltpu.SemaphoreType.DMA((4,))],
        compiler_params=pltpu.CompilerParams(vmem_limit_bytes=60 * 1024 * 1024, dimension_semantics=("arbitrary",),
                                             collective_id=1, has_side_effects=True),
        cost_estimate=pl.CostEstimate(flops=ROWS * DM * 4096, bytes_accessed=32 << 20, transcendentals=0),
        name="qkv",
    )(hidden, gb, cos_t, s1_t, s2_t, w_q, w_k, w_v)


def attn_kernel(events, lens_ref, q_ref, kc_ref, vc_ref, qh_ref, kn_ref, vn_ref, hid_ref, wo_ref, out_ref,
                kbuf, vbuf, pos, acc, st, drecv, dst, cst, sst, xrecv, xst, pout, yrecv, obuf, wo, qown, knb, vnb, knf, vnf, hid,
                ctxf, lhs, stage, scr, sms, csem, lsem, osem, ssem, rsem):
    i = pl.program_id(0)
    dp = lax.axis_index("dp")
    y = lax.axis_index("tp")
    s = lax.axis_index("sp")
    x = s // 2
    c = lax.rem(s, 2)
    nx, nc, ny = 1 - x, 1 - c, 1 - y
    dev_c = (dp, y, 2 * x + nc)
    dev_x = (dp, y, 2 * nx + c)
    dev_y = (dp, ny, s)
    own, own_x, own_y, own_xy = 2 * x + y, 2 * nx + y, 2 * x + ny, 2 * nx + ny
    base = s * 128

    def remote(kind, ch, src, dst_, dev):
        return pltpu.make_async_remote_copy(src_ref=src, dst_ref=dst_, send_sem=ssem.at[kind, ch], recv_sem=rsem.at[kind, ch],
                                            device_id=dev, device_id_type=MESH)

    locals_ = [
        (wo_ref.at[:, pl.ds(pl.multiple_of(c * HALF, HALF), HALF)], wo), (qh_ref.at[:, x, c], qown), (kn_ref.at[x, c], knb), (vn_ref.at[x, c], vnb), (hid_ref.at[x, y, :, pl.ds(pl.multiple_of(c * HALF, HALF), HALF)], hid),
    ]

    def local_copy(n):
        a, b = locals_[n]
        return pltpu.make_async_copy(a, b, lsem.at[n])

    def cache_copies(t):
        b = lax.rem(t, NBUF)
        blk = pl.ds(t * STEP, STEP)
        return (pltpu.make_async_copy(kc_ref.at[:, :, blk], kbuf.at[b], csem.at[0, b]),
                pltpu.make_async_copy(vc_ref.at[:, :, blk], vbuf.at[b], csem.at[1, b]))

    @pl.when(i == 0)
    def _():
        for t in range(NBUF - 1):
            for cp in cache_copies(t):
                cp.start()

    @pl.when(i < NSTEP - NBUF + 1)
    def _():
        for cp in cache_copies(i + NBUF - 1):
            cp.start()

    @pl.when(i == 0)
    def _():
        sem = pltpu.get_barrier_semaphore()
        for dev in (dev_c, dev_x, dev_y):
            pl.semaphore_signal(sem, inc=1, device_id=dev, device_id_type=MESH)
        col = lax.broadcasted_iota(jnp.int32, (48, 512), 1)
        row = lax.broadcasted_iota(jnp.int32, (48, 512), 0)
        jj = (row >> 3) * 4 + (row & 3)
        head = (jj >= 6).astype(jnp.int32) + (jj >= 12).astype(jnp.int32) + (jj >= 18).astype(jnp.int32)
        pos[...] = jnp.where((col & 3) == head, col >> 2, 1 << 20)
        pl.semaphore_wait(sem, 3)

    @pl.when(i == 1)
    def _():
        for n in range(len(locals_)):
            local_copy(n).start()

    lane = lax.broadcasted_iota(jnp.int32, (48, D), 1)
    low = (lax.broadcasted_iota(jnp.int32, (48, D), 0) & 7) < 4
    low1 = (lax.broadcasted_iota(jnp.int32, (48, 1), 0) & 7) < 4

    @pl.when(i < NSTEP)
    def _():
        for cp in cache_copies(i):
            cp.wait()
        k_ref = kbuf.at[lax.rem(i, NBUF)]
        for xo in range(2):
            for co in range(2):
                for pp in range(STEP // 2):
                    q48 = q_ref[:, xo, co, pp * 8:(pp + 1) * 8, :].reshape(48, D)
                    qbd = jnp.concatenate([jnp.where(low, q48, 0.0), jnp.where(low, 0.0, q48)], axis=1).astype(BF16)
                    kk = jnp.concatenate([k_ref[xo, co, 2 * pp], k_ref[xo, co, 2 * pp + 1]], axis=1)
                    sc = lax.dot_general(qbd, kk, (((1,), (1,)), ((), ())), preferred_element_type=F32)
                    r0 = (2 * xo + co) * OWN + i * STEP + 2 * pp
                    lenv = jnp.where(low1, lens_ref[r0] - base, lens_ref[r0 + 1] - base)
                    scr[(xo * 2 + co) * (STEP // 2) + pp] = jnp.where(pos[...] < lenv, sc * SCALE2, NEG)

    @pl.when(i < NSTEP)
    def _():
        v_ref = vbuf.at[lax.rem(i, NBUF)]
        ch = i // SPC
        within = lax.rem(i, SPC)
        for xo in range(2):
            for co in range(2):
                stats = jnp.where(within == 0, 0.0, st[ch, co, xo])
                for pp in range(STEP // 2):
                    sc = scr[(xo * 2 + co) * (STEP // 2) + pp]
                    m = jnp.maximum(jnp.max(sc, axis=1, keepdims=True), FLOOR)
                    w = jnp.exp2(sc - m)
                    l = jnp.sum(w, axis=1, keepdims=True)
                    vv = jnp.concatenate([v_ref[xo, co, 2 * pp], v_ref[xo, co, 2 * pp + 1]], axis=1)
                    o = jnp.dot(w.astype(BF16), vv, preferred_element_type=F32)
                    at = pl.multiple_of((i * STEP + 2 * pp) * G, 2 * G)
                    acc[co, xo, pl.ds(at, 2 * G), :] = jnp.where(low, o[:, :D], o[:, D:])
                    idx = within * (STEP // 2) + pp
                    stats = jnp.where(lane == idx, m, jnp.where(lane == idx + NP, l, stats))
                st[ch, co, xo] = stats

    def pick(block, n):
        return jnp.sum(jnp.where(lane == n, block, 0.0), axis=1, keepdims=True)

    def sums(block):
        return pltpu.roll(block, D - NP, 1)

    def crows(ch):
        return pl.ds(ch * CR * G, CR * G)

    def c_acc(ch):
        return remote(KD, ch, acc.at[nc, :, crows(ch)], drecv.at[:, crows(ch)], dev_c)

    def c_st(ch):
        return remote(KDS, ch, st.at[ch, nc], dst.at[ch], dev_c)

    def x_acc(ch):
        return remote(KX, ch, acc.at[c, nx, crows(ch)], xrecv.at[crows(ch)], dev_x)

    def x_st(ch):
        return remote(KXS, ch, sst.at[ch], xst.at[ch], dev_x)

    def y_part(ch):
        return remote(KY, ch, pout.at[ch % 4, ny], yrecv.at[ch], dev_y)

    def ctx_copy(ch):
        return remote(KC, ch, ctxf.at[ch, c], ctxf.at[ch, c], dev_c)

    def ctx_in(ch):
        return remote(KC, ch, ctxf.at[ch, nc], ctxf.at[ch, nc], dev_c)

    def piece(half, owner, ch):
        return obuf.at[half, owner, pl.ds(ch * CR, CR)]

    def gather(kind, ch, dev, half, owner):
        return remote(kind, ch, piece(half, owner, ch), piece(half, owner, ch), dev)

    def ev_core(ch):
        c_acc(ch).start()
        c_st(ch).start()

    def pairs(ch, body, init):
        def four(t, carry):
            for u in range(NP):
                n = t * NP + u
                rows = pl.ds((ch * CR + 2 * n) * G, 2 * G)
                carry = body(n, rows, carry)
            return carry
        return four(0, init)

    def spread(ref, ch, n):
        krows = pl.ds((ch * CR + 2 * n) * KV, 2 * KV)
        rr = lax.broadcasted_iota(jnp.int32, (48, 8), 0)
        cc = lax.broadcasted_iota(jnp.int32, (48, 8), 1)
        first = ((cc & 3) * 6)
        jj = (rr >> 3) * 4 + (rr & 3)
        hot = ((jj >= first) & (jj < first + 6) & (((rr >> 2) & 1) == (cc >> 2))).astype(F32)
        return jnp.dot(hot, ref[krows, :], preferred_element_type=F32)

    def ev_x(ch):
        c_acc(ch).wait_recv()
        c_st(ch).wait_recv()

        def merge(xo):
            a, b = st[ch, c, xo], dst[ch, xo]
            m = jnp.maximum(a, b)
            fa, fb = jnp.exp2(a - m), jnp.exp2(b - m)
            both = jnp.where(lane < NP, m, pltpu.roll(sums(a) * fa + sums(b) * fb, NP, 1))
            if xo is x:
                cst[ch] = both
            else:
                small = both[:8]
                for g in range(1, 6):
                    small = jnp.where(lane[:8] >= 16 * g, pltpu.roll(both[8 * g:8 * g + 8], 16 * g, 1), small)
                sst[ch] = small

            def body(n, rows, carry):
                acc[c, xo, rows, :] = acc[c, xo, rows, :] * pick(fa, n) + drecv[xo, rows, :] * pick(fb, n)
                return carry
            pairs(ch, body, 0)
        merge(nx)
        x_acc(ch).start()
        x_st(ch).start()
        merge(x)

    def ev_self(ch):
        if ch == 0:
            for n in range(len(locals_)):
                local_copy(n).wait()
            knf[...] = knb[...].astype(F32)
            vnf[...] = vnb[...].astype(F32)

        def body(n, rows, out):
            qq = qown[:, pl.ds((ch * CR + 2 * n) * 4, 8), :].reshape(48, D)
            val = jnp.sum(qq.astype(BF16).astype(F32) * spread(knf, ch, n), axis=1, keepdims=True)
            return jnp.where(lane == n, val, out)
        sms[ch] = pairs(ch, body, jnp.zeros((48, D), F32)) * SCALE2

    def ev_ctx(ch):
        x_acc(ch).wait_recv()
        x_st(ch).wait_recv()
        a, z, got = cst[ch], sms[ch], xst[ch]
        b = jnp.concatenate([got] + [pltpu.roll(got, D - 16 * g, 1) for g in range(1, 6)], axis=0)
        m = jnp.maximum(jnp.maximum(a, b), z)
        fa, fb, fs = jnp.exp2(a - m), jnp.exp2(b - m), jnp.exp2(z - m)
        tot = sums(a) * fa + sums(b) * fb + fs
        fa, fb, fs = fa / tot, fb / tot, fs / tot

        def body(n, rows, carry):
            ctx = acc[c, x, rows, :] * pick(fa, n) + xrecv[rows, :] * pick(fb, n) + pick(fs, n) * spread(vnf, ch, n)
            for k in range(3):
                lo, hi = ctx[16 * k:16 * k + 8], ctx[16 * k + 8:16 * k + 16]
                at = n * 48 + 8 * k
                ctxf[ch, c, pl.ds(at, 8), :] = jnp.where(low[:8], lo, pltpu.roll(hi, 4, 0))
                ctxf[ch, c, pl.ds(at + G, 8), :] = jnp.where(low[:8], pltpu.roll(lo, 4, 0), hi)
            return carry
        pairs(ch, body, 0)
        ctx_copy(ch).start()

    def ev_proj(group):
        m = len(group)
        for g, ch in enumerate(group):
            ctx_in(ch).wait_recv()
            for j in range(G):
                for half in range(2):
                    lhs[pl.ds((2 * g + half) * CR, CR), j * D:(j + 1) * D] = ctxf[ch, half, pl.ds(j, CR, G), :].astype(BF16)
            if ch >= 4:
                y_part(ch - 4).wait_send()

        def mm(n, _):
            cols = pl.ds(pl.multiple_of(n * 512, 512), 512)
            part = jnp.dot(lhs[:m * 2 * CR], wo[:, cols], preferred_element_type=F32)
            for g, ch in enumerate(group):
                for half in range(2):
                    pout[ch % 4, half, :, cols] = part[(2 * g + half) * CR:(2 * g + half + 1) * CR]
            return 0
        lax.fori_loop(0, HALF // 512, mm, 0)
        for ch in group:
            y_part(ch).start()

    def ev_sum(ch):
        y_part(ch).wait_recv()
        rows = pl.ds(ch * CR, CR)

        def body(n, _):
            cols = pl.ds(pl.multiple_of(n * 512, 512), 512)
            obuf[c, own, rows, cols] = pout[ch % 4, y, :, cols] + yrecv[ch, :, cols] + hid[rows, cols].astype(F32)
            return 0
        lax.fori_loop(0, HALF // 512, body, 0)
        gather(KFX, ch, dev_x, c, own).start()
        gather(KFY, ch, dev_y, c, own).start()
        gather(KFC, ch, dev_c, c, own).start()

    def forward(ch):
        if ch in XFWD:
            return gather(KGY, ch, dev_x, c, own_y)
        return gather(KGY, ch, dev_y, c, own_x)

    def ev_fwd(ch):
        gather(KFX, ch, dev_x, c, own_x).wait_recv()
        if ch not in XFWD:
            forward(ch).start()
        gather(KGCX, ch, dev_c, c, own_x).start()
        gather(KFY, ch, dev_y, c, own_y).wait_recv()
        if ch in XFWD:
            forward(ch).start()
        gather(KGCY, ch, dev_c, c, own_y).start()

    def ev_last(ch):
        gather(KGY, ch, dev_y, c, own_xy).wait_recv()
        gather(KGCD, ch, dev_c, c, own_xy).start()

    def out_copy(ch):
        return pltpu.make_async_copy(stage.at[ch % 2], out_ref.at[:, pl.ds(ch * CR, CR)], osem.at[ch % 2])

    def ev_out(ch):
        gather(KFC, ch, dev_c, nc, own).wait_recv()
        gather(KGCX, ch, dev_c, nc, own_x).wait_recv()
        gather(KGCY, ch, dev_c, nc, own_y).wait_recv()
        gather(KGCD, ch, dev_c, nc, own_xy).wait_recv()
        if ch >= 2:
            out_copy(ch - 2).wait()
        rows = pl.ds(ch * CR, CR)

        def body(n, _):
            for half in range(2):
                for q4 in range(4):
                    stage[ch % 2, n, :, half * HALF + q4 * 512:half * HALF + (q4 + 1) * 512] = obuf[half, n, rows, q4 * 512:(q4 + 1) * 512].astype(BF16)
            return 0
        lax.fori_loop(0, 4, body, 0)
        out_copy(ch).start()

    def ev_drain(ch):
        c_acc(ch).wait_send()
        c_st(ch).wait_send()
        x_acc(ch).wait_send()
        x_st(ch).wait_send()
        ctx_copy(ch).wait_send()
        if ch >= NCH - 4:
            y_part(ch).wait_send()
        for kind, dev, owner in ((KFX, dev_x, own), (KFY, dev_y, own), (KFC, dev_c, own),
                                 (KGCX, dev_c, own_x), (KGCY, dev_c, own_y), (KGCD, dev_c, own_xy)):
            gather(kind, ch, dev, c, owner).wait_send()
        forward(ch).wait_send()
        if ch >= NCH - 2:
            out_copy(ch).wait()

    table = {"core": ev_core, "x": ev_x, "self": ev_self, "ctx": ev_ctx, "proj": ev_proj, "sum": ev_sum, "fwd": ev_fwd, "last": ev_last, "out": ev_out, "drain": ev_drain}
    for when, names in events:
        @pl.when(i == when)
        def _(names=names):
            for name, ch in names:
                table[name](ch)


def schedule():
    order = {name: n for n, name in enumerate(OFFS)}
    plan = []
    for ch in range(NCH):
        first = SPC * (ch + 1) - 1
        for name, off in OFFS.items():
            if name != "proj":
                plan.append((first + off, order[name], name, ch))
    for group in GROUPS:
        plan.append((SPC * (group[-1] + 1) - 1 + OFFS["proj"], order["proj"], "proj", group))
    plan.sort()
    steps = {}
    for at, _, name, arg in plan:
        steps.setdefault(min(int(at), NSTEP), []).append((name, arg))
    steps[NSTEP] += [("drain", ch) for ch in range(NCH)]
    return tuple((at, tuple(steps[at])) for at in sorted(steps))


def attend(lengths, q, k_cache, v_cache, kn, vn, hidden, w_o):
    hbm = pl.BlockSpec(memory_space=pl.ANY)
    hold = NSTEP - 1
    return pl.pallas_call(
        functools.partial(attn_kernel, schedule()),
        grid=(NSTEP + 1,),
        out_shape=jax.ShapeDtypeStruct((4, OWN, DM), BF16),
        in_specs=[pl.BlockSpec(memory_space=pltpu.SMEM),
                  pl.BlockSpec((6, 2, 2, STEP * 4, D), lambda i: (0, 0, 0, jnp.minimum(i, hold), 0)),
                  hbm, hbm, hbm, hbm, hbm, hbm, hbm],
        out_specs=hbm,
        scratch_shapes=[
            pltpu.VMEM((NBUF, 2, 2, STEP, 512, D), BF16),
            pltpu.VMEM((NBUF, 2, 2, STEP, 512, D), BF16),
            pltpu.VMEM((48, 512), jnp.int32),
            pltpu.VMEM((2, 2, OWN * G, D), F32),
            pltpu.VMEM((NCH, 2, 2, 48, D), F32),
            pltpu.VMEM((2, OWN * G, D), F32),
            pltpu.VMEM((NCH, 2, 48, D), F32),
            pltpu.VMEM((NCH, 48, D), F32),
            pltpu.VMEM((NCH, 8, D), F32),
            pltpu.VMEM((OWN * G, D), F32),
            pltpu.VMEM((NCH, 8, D), F32),
            pltpu.VMEM((4, 2, CR, HALF), F32),
            pltpu.VMEM((NCH, CR, HALF), F32),
            pltpu.VMEM((2, 4, OWN, HALF), F32),
            pltpu.VMEM((G * D, HALF), BF16),
            pltpu.VMEM((6, OWN * 4, D), F32),
            pltpu.VMEM((OWN * KV, D), BF16),
            pltpu.VMEM((OWN * KV, D), BF16),
            pltpu.VMEM((OWN * KV, D), F32),
            pltpu.VMEM((OWN * KV, D), F32),
            pltpu.VMEM((OWN, HALF), BF16),
            pltpu.VMEM((NCH, 2, CR * G, D), F32),
            pltpu.VMEM((4 * CR, G * D), BF16),
            pltpu.VMEM((2, 4, CR, DM), BF16),
            pltpu.VMEM((2 * STEP, 48, 512), F32),
            pltpu.VMEM((NCH, 48, D), F32),
            pltpu.SemaphoreType.DMA((2, NBUF)),
            pltpu.SemaphoreType.DMA((5,)),
            pltpu.SemaphoreType.DMA((2,)),
            pltpu.SemaphoreType.DMA((NKIND, NCH)),
            pltpu.SemaphoreType.DMA((NKIND, NCH)),
        ],
        compiler_params=pltpu.CompilerParams(vmem_limit_bytes=67043328, collective_id=0, has_side_effects=True,
                                             dimension_semantics=("arbitrary",)),
        cost_estimate=pl.CostEstimate(flops=10 ** 10, bytes_accessed=170 << 20, transcendentals=0),
        name="attend",
    )(lengths, q, k_cache, v_cache, q, kn, vn, hidden, w_o)


def solution(mesh):
    def local_step(hidden, ln_gain, ln_bias, w_q, w_k, w_v, w_o, k_cache, v_cache, lengths):
        half = D // 4
        inv = 10000.0 ** (-2.0 * jnp.arange(half, dtype=F32) / (D // 2))
        ang = lengths.astype(F32)[:, None] * inv
        cos, sin = jnp.cos(ang), jnp.sin(ang)
        zero = jnp.zeros_like(sin)
        cos_t = jnp.concatenate([cos, cos, jnp.ones((ROWS, 2 * half), F32)], axis=1)
        s1_t = jnp.concatenate([-sin, zero, zero, zero], axis=1)
        s2_t = jnp.concatenate([zero, sin, zero, zero], axis=1)
        gb = jnp.stack([1.0 + ln_gain.astype(F32), ln_bias.astype(F32)])
        q, kn, vn = project(hidden, gb, cos_t, s1_t, s2_t, w_q, w_k, w_v)
        out = attend(lengths, q.reshape(6, 2, 2, OWN * 4, D),
                     k_cache.reshape(2, 2, OWN, 512, D), v_cache.reshape(2, 2, OWN, 512, D),
                     kn.reshape(2, 2, OWN * KV, D), vn.reshape(2, 2, OWN * KV, D),
                     hidden.reshape(2, 2, OWN, DM), w_o)
        return out.reshape(ROWS, DM), kn.reshape(ROWS, KV, D), vn.reshape(ROWS, KV, D)

    row_spec = P('dp', None)
    cache_spec = P('dp', 'sp', 'tp', None)
    head_spec = P('dp', 'tp', None)
    return jax.shard_map(local_step, mesh=mesh, in_specs=(row_spec, P(None), P(None), P(None, 'tp'), P(None, 'tp'), P(None, 'tp'), P('tp', None), cache_spec, cache_spec, P('dp')), out_specs=(row_spec, head_spec, head_spec), check_vma=False)
```
